128 devices in a mesh: slc: 64 (over x_hi, y, z, core), col: 2 (over x_lo).
Axes of the slice: x: 4 (x_hi: 2, x_lo: 2; x = x_hi * 2 + x_lo), y: 4, z: 4, core: 2. Of those that a mesh axis runs over, the one named last changes fastest.
Arguments:
- basis: bfloat16 [64, 2, 1152, 3456], P('slc', None, None, 'col'), may hold values from -6 to 6
- picks: int32 [64, 608], P('slc', 'col'), may hold values from 0 to 1727, as said below
- coil_maps: bfloat16 [128, 64, 2, 32, 128], P('slc'), may hold values from -6 to 6
Outputs:
- mapped: bfloat16 [128, 64, 2, 32, 128], P('slc', None, None, 'col')
The draws below stay inside these ranges and needn't reach their ends.
Inputs may be any that keep to these rules, and one draw needn't show every extreme that they name: `picks`: for each slice, the entries in each of the 2 blocks of 304 positions are distinct offsets within the corresponding block of 1728 calibration windows.
All inputs are finite; a program needn't handle non-finite values.
Results may differ from the reference program's by a relative error of at most 0.0049.
Values may be sent and summed in bfloat16 or wider, within the bound.
No kernel may reach another device: no remote copies, remote signals or barrier semaphores. Data moves between devices by JAX's collectives and lax.ppermute only.
A program may use at most 448 MiB of HBM per device.

```python
import math
import jax
import jax.numpy as jnp
from jax import lax

COILS = 32
KSIZE = 6
NCOL = 3456
RANK = 608
IMG = 128
ROWS = 1152
SLICES = 64
N_COL = 2


def draw_picks(key, part):
    block_cols = NCOL // N_COL
    keep_cols = RANK // N_COL
    keys = jax.random.split(jax.random.fold_in(key, 7), SLICES * N_COL)
    chosen = jax.vmap(lambda one_key: jax.random.permutation(one_key, block_cols)[:keep_cols])(keys)
    return chosen.reshape(SLICES, RANK).astype(jnp.int32)


def block_levels(own_key, shape, shards, smallest, high):
    def one(position, parts):
        heights = jax.random.uniform(jax.random.fold_in(jax.random.fold_in(own_key, 6), position), (parts,), jnp.float32, smallest / len(shards), high / len(shards))
        return jnp.repeat(jnp.exp(heights), shape[position] // parts).reshape((-1,) + (1,) * (len(shape) - position - 1))

    factor_of = one(*shards[0])
    for cut in shards[1:]:
        factor_of = factor_of * one(*cut)
    return factor_of


def scatter_about(rng, shape, scale, bound, pieces=(), held_as=jnp.bfloat16):
    values = scale * jax.random.normal(rng, shape, jnp.float32)
    if pieces:
        values = values * block_levels(rng, shape, pieces, -0.22, 0.18)
    return jnp.clip(values, -bound, bound).astype(held_as)


def setup_inputs(seed: int = 0) -> dict:
    key_list = jax.random.split(jax.random.key(seed), 4)
    basis = scatter_about(key_list[0], (SLICES, 2, ROWS, NCOL), 1.0, 6.0, ((0, 64), (3, 2)))
    picks = draw_picks(jax.random.fold_in(key_list[3], 71), 0)
    coil_maps = scatter_about(key_list[2], (IMG, SLICES, 2, COILS, IMG), 1.0, 6.0, ((0, 64),))
    return dict(basis=basis, picks=picks, coil_maps=coil_maps)


def phase_tables(span, length):
    centre = (span - 1) // 2
    offsets = jnp.arange(span).astype(jnp.int32) - centre
    columns = jnp.arange(length).astype(jnp.int32)
    turns = (offsets[:, None] * columns[None, :]) % length
    angles = turns.astype(jnp.float32) * (2.0 * math.pi / length)
    return jnp.cos(angles), jnp.sin(angles)


def shift_table(count):
    first = jnp.arange(count).astype(jnp.int32)[:, None, None]
    second = jnp.arange(count).astype(jnp.int32)[None, :, None]
    target = jnp.arange(2 * count - 1).astype(jnp.int32)[None, None, :]
    return (second - first + count - 1 == target).astype(jnp.float32)


def slice_gram(values_in):
    real_part = jnp.dot(values_in[0], values_in[0].T, preferred_element_type=jnp.float32) + jnp.dot(values_in[1], values_in[1].T, preferred_element_type=jnp.float32)
    imag_part = jnp.dot(values_in[1], values_in[0].T, preferred_element_type=jnp.float32) - jnp.dot(values_in[0], values_in[1].T, preferred_element_type=jnp.float32)
    return jnp.stack([real_part, imag_part])


def kernel_sums(gram):
    blocks = gram.reshape(2, COILS, KSIZE, KSIZE, COILS, KSIZE, KSIZE)
    shifts = shift_table(KSIZE)
    return jnp.einsum("rcaxdby,abp,xyq->rcdpq", blocks, shifts, shifts, precision=lax.Precision.HIGHEST)


def column_transform(kernels, cos_table, sin_table, factor):
    def apply_table(values_in, table):
        return jnp.einsum("cdpq,qy->ycdp", values_in, table, precision=lax.Precision.HIGHEST)
    real_part = apply_table(kernels[0], cos_table) - apply_table(kernels[1], sin_table)
    imag_part = apply_table(kernels[0], sin_table) + apply_table(kernels[1], cos_table)
    return (jnp.stack([real_part, imag_part], axis=1) * factor).astype(jnp.bfloat16)


def apply_maps(rows_q, maps_one, cos_table, sin_table):
    kernel_f = rows_q.astype(jnp.float32)
    maps_f = maps_one.astype(jnp.float32)

    def product(left_op, right_op):
        return jnp.einsum("ycdp,ydx->ycpx", left_op, right_op, precision=lax.Precision.HIGHEST)
    mixed_real = product(kernel_f[:, 0], maps_f[:, 0]) - product(kernel_f[:, 1], maps_f[:, 1])
    mixed_imag = product(kernel_f[:, 0], maps_f[:, 1]) + product(kernel_f[:, 1], maps_f[:, 0])

    def apply_table(values_in, table):
        return jnp.einsum("ycpx,px->ycx", values_in, table, precision=lax.Precision.HIGHEST)
    out_real = apply_table(mixed_real, cos_table) - apply_table(mixed_imag, sin_table)
    out_imag = apply_table(mixed_real, sin_table) + apply_table(mixed_imag, cos_table)
    return jnp.stack([out_real, out_imag], axis=1).astype(jnp.bfloat16)


def reference(basis, picks, coil_maps):
    block_cols = NCOL // N_COL
    keep_cols = RANK // N_COL
    offsets = (jnp.arange(RANK).astype(jnp.int32) // keep_cols) * block_cols
    span = 2 * KSIZE - 1
    cos_table, sin_table = phase_tables(span, IMG)
    factor = 1.0 / (2.0 * RANK * KSIZE * KSIZE)
    maps_first = jnp.transpose(coil_maps, (1, 0, 2, 3, 4))

    def per_slice(inputs):
        values_in, columns, maps_one = inputs
        picked = jnp.take(values_in, columns.astype(jnp.int32) + offsets, axis=2)
        gram = slice_gram(picked)
        kernels = kernel_sums(gram)
        rows_q = column_transform(kernels, cos_table, sin_table, factor)
        return apply_maps(rows_q, maps_one, cos_table, sin_table)

    results = lax.map(per_slice, (basis, picks, maps_first))
    return jnp.transpose(results, (1, 0, 2, 3, 4))
```

```python
import math

import jax
import jax.numpy as jnp
import numpy as np
from jax import lax
from jax.experimental import pallas as pl
from jax.experimental.pallas import tpu as pltpu
from jax.sharding import PartitionSpec as P

COILS = 32
KSIZE = 6
RANK = 608
IMG = 128
SPAN = 2 * KSIZE - 1
LANES = 128
AROWS = KSIZE * COILS
GROUPS = 4
CHUNK_COILS = 16
WIDE = 384
YBLOCK = 4
SBLOCK = 8


def gram_kernel(picks_ref, basis_ref, keep_ref, send_ref, onehot, rows, left, right):
    step = pl.program_id(0)
    windows = basis_ref.shape[-1]
    used = picks_ref.shape[-1]
    chunk = CHUNK_COILS * KSIZE * KSIZE

    @pl.when(step == 0)
    def _():
        wanted = jnp.concatenate(
            [picks_ref[...], jnp.full((1, WIDE - used), -1, jnp.int32)], axis=1
        )
        index = lax.broadcasted_iota(jnp.int32, (windows, WIDE), 0)
        onehot[...] = jnp.where(index == wanted, 1.0, 0.0).astype(jnp.bfloat16)
        right[:, AROWS:, :] = jnp.zeros(
            (2, right.shape[1] - AROWS, right.shape[2]), jnp.bfloat16
        )

    picked = jnp.dot(basis_ref[0], onehot[...], preferred_element_type=jnp.float32)
    for tile in range(WIDE // LANES):
        rows[tile] = picked[:, tile * LANES : (tile + 1) * LANES]
    part = step // 2
    first_coil = (step % 2) * CHUNK_COILS
    for a in range(KSIZE):
        row = pl.multiple_of(a * COILS + first_coil, CHUNK_COILS)
        for b in range(KSIZE):
            for tile in range(WIDE // LANES):
                block = rows[
                    tile, pl.ds(a * KSIZE + b, CHUNK_COILS, stride=KSIZE * KSIZE), :
                ].astype(jnp.bfloat16)
                lane = b * WIDE + tile * LANES
                left[part, pl.ds(row, CHUNK_COILS), lane : lane + LANES] = block
                right[part, pl.ds(row, CHUNK_COILS), lane : lane + LANES] = block

    @pl.when(step == 3)
    def _():
        def against(q, part):
            depth = (KSIZE - q) * WIDE
            lhs = left[:, :, :depth].reshape(2 * AROWS, depth)
            return lax.dot_general(
                lhs,
                right[part, :, q * WIDE :],
                (((1,), (1,)), ((), ())),
                preferred_element_type=jnp.float32,
            )

        pad = jnp.zeros((COILS, WIDE - right.shape[1]), jnp.float32)
        for q in range(KSIZE):
            with_real = against(q, 0)
            with_imag = against(q, 1)
            pair = (
                with_real[:AROWS] + with_imag[AROWS:],
                with_real[AROWS:] - with_imag[:AROWS],
            )
            for part in range(2):
                total = None
                for a in range(KSIZE):
                    block = jnp.concatenate(
                        [pair[part][a * COILS : (a + 1) * COILS], pad], axis=1
                    )
                    shift = (KSIZE - 1 - a) * COILS
                    moved = pltpu.roll(block, shift, 1) if shift else block
                    total = moved if total is None else total + moved
                keep_ref[q, part] = total
                send_ref[q, part] = total.astype(jnp.bfloat16)


def partial_kernels(basis, picks):
    parts, rows, windows = basis.shape
    used = picks.shape[1]
    chunk = CHUNK_COILS * KSIZE * KSIZE
    return pl.pallas_call(
        gram_kernel,
        grid=(2 * rows // chunk,),
        in_specs=[
            pl.BlockSpec((1, used), lambda i: (0, 0)),
            pl.BlockSpec((1, chunk, windows), lambda i: (i // 2, i % 2, 0)),
        ],
        out_specs=[
            pl.BlockSpec((KSIZE, 2, COILS, WIDE), lambda i: (0, 0, 0, 0)),
            pl.BlockSpec((KSIZE, 2, COILS, WIDE), lambda i: (0, 0, 0, 0)),
        ],
        out_shape=[
            jax.ShapeDtypeStruct((KSIZE, 2, COILS, WIDE), jnp.float32),
            jax.ShapeDtypeStruct((KSIZE, 2, COILS, WIDE), jnp.bfloat16),
        ],
        scratch_shapes=[
            pltpu.VMEM((windows, WIDE), jnp.bfloat16),
            pltpu.VMEM((WIDE // LANES, chunk, LANES), jnp.float32),
            pltpu.VMEM((2, AROWS, KSIZE * WIDE), jnp.bfloat16),
            pltpu.VMEM((2, 256, KSIZE * WIDE), jnp.bfloat16),
        ],
        compiler_params=pltpu.CompilerParams(
            dimension_semantics=("arbitrary",), vmem_limit_bytes=40 * 2**20
        ),
        name="partial_kernels",
    )(picks, basis)


def lane_pattern(values):
    return np.tile(np.repeat(np.asarray(values, np.float32), COILS), 2)


def transform_table():
    half = IMG // 4
    table = np.zeros((half, 16, LANES), np.float32)
    for first in range(half):
        for q in range(1, KSIZE):
            lanes_y = np.repeat(2 * first + np.arange(2), LANES // 2)
            angle = 2.0 * math.pi * ((q * lanes_y) % IMG) / IMG
            table[first, q - 1] = np.cos(angle)
            table[first, KSIZE - 2 + q] = np.sin(angle)
    return table


def transform_kernel(half_ref, keep_ref, got_ref, table_ref, out_ref, whole, turned, terms):
    coil_share = COILS // 2

    @pl.when(pl.program_id(0) == 0)
    def _():
        factor = 1.0 / (2.0 * RANK * KSIZE * KSIZE)
        summed = (keep_ref[...] + got_ref[...].astype(jnp.float32)) * factor
        whole[...] = summed
        turned[...] = summed.reshape(2 * KSIZE * COILS, WIDE).T
        own = pl.multiple_of(half_ref[0] * coil_share, coil_share)
        lane = lax.broadcasted_iota(jnp.int32, (coil_share, LANES), 1)
        group = lane // COILS
        swap_sign = jnp.where(group % 2 == 0, 1.0, -1.0)

        def spread(q, p):
            tile, slot = divmod(p, LANES // COILS)
            blocks = [
                whole[q, part, pl.ds(own, coil_share), tile * LANES : (tile + 1) * LANES]
                for part in range(2)
            ]
            result = None
            for target in range(GROUPS):
                shift = (target - slot) % GROUPS * COILS
                moved = blocks[target % 2]
                moved = pltpu.roll(moved, shift, 1) if shift else moved
                result = moved if result is None else jnp.where(group == target, moved, result)
            return result

        def flipped(q, p):
            row = pl.multiple_of((SPAN - 1 - p) * COILS + own, coil_share)
            tile = turned[pl.ds(row, coil_share), (q // 2) * LANES : (q // 2 + 1) * LANES]
            other = pltpu.roll(tile, LANES // 2, 1)
            upper = lane >= LANES // 2
            doubled = jnp.where(upper, other, tile) if q % 2 == 0 else jnp.where(upper, tile, other)
            return doubled * swap_sign

        def terms_of(p):
            made = [spread(0, p)]
            sines = []
            for q in range(1, KSIZE):
                forward = spread(q, p)
                backward = flipped(q, p)
                made.append(forward + backward)
                gap = pltpu.roll(forward - backward, COILS, 1)
                sines.append(gap * -swap_sign)
            return made + sines

        centre = KSIZE - 1
        for index, term in enumerate(terms_of(centre)):
            terms[index, :coil_share] = term
        for offset in range(1, KSIZE):
            upper = terms_of(centre + offset)
            lower = terms_of(centre - offset)
            for index in range(2 * KSIZE - 1):
                even = offset * coil_share
                odd = (offset + KSIZE - 1) * coil_share
                terms[index, even : even + coil_share] = upper[index] + lower[index]
                terms[index, odd : odd + coil_share] = upper[index] - lower[index]

    for local in range(YBLOCK):
        weights = [
            jnp.broadcast_to(table_ref[local, index : index + 1, :], (coil_share, LANES))
            for index in range(2 * KSIZE - 2)
        ]
        for block in range(SPAN):
            rows = slice(block * coil_share, (block + 1) * coil_share)
            even = terms[0, rows]
            odd = None
            for q in range(1, KSIZE):
                piece = (
                    terms[q, rows] * weights[q - 1]
                    + terms[KSIZE - 1 + q, rows] * weights[KSIZE - 2 + q]
                )
                if q % 2 == 0:
                    even = even + piece
                else:
                    odd = piece if odd is None else odd + piece
            out_ref[0, local, rows, :] = (even + odd).astype(jnp.bfloat16)
            out_ref[1, local, rows, :] = (even - odd).astype(jnp.bfloat16)


def column_rows(half, keep, got):
    blocks = IMG // 4
    rows = SPAN * COILS // 2
    whole = lambda i, h: (0, 0, 0, 0)
    return pl.pallas_call(
        transform_kernel,
        grid_spec=pltpu.PrefetchScalarGridSpec(
            num_scalar_prefetch=1,
            grid=(blocks // YBLOCK,),
            in_specs=[
                pl.BlockSpec(keep.shape, whole),
                pl.BlockSpec(got.shape, whole),
                pl.BlockSpec((YBLOCK, 16, LANES), lambda i, h: (i, 0, 0)),
            ],
            out_specs=pl.BlockSpec((2, YBLOCK, rows, LANES), lambda i, h: (0, i, 0, 0)),
            scratch_shapes=[
                pltpu.VMEM((KSIZE, 2, COILS, WIDE), jnp.float32),
                pltpu.VMEM((WIDE, 2 * KSIZE * COILS), jnp.float32),
                pltpu.VMEM((2 * KSIZE - 1, rows, LANES), jnp.float32),
            ],
        ),
        out_shape=jax.ShapeDtypeStruct((2, blocks, rows, LANES), jnp.bfloat16),
        compiler_params=pltpu.CompilerParams(dimension_semantics=("arbitrary",)),
        name="column_rows",
    )(half, keep, got, jnp.asarray(transform_table()))


def phase_table():
    table = np.zeros((16, IMG), np.float32)
    for p in range(1, KSIZE):
        angle = 2.0 * math.pi * ((p * np.arange(IMG)) % IMG) / IMG
        table[p - 1] = np.cos(angle)
        table[KSIZE - 2 + p] = np.sin(angle)
    return table


def apply_kernel(rows_ref, maps_ref, table_ref, out_ref):
    coil_share = COILS // 2
    waves = [
        jnp.broadcast_to(table_ref[index : index + 1, :], (coil_share, IMG))
        for index in range(2 * KSIZE - 2)
    ]
    blank = jnp.zeros((2 * COILS, 2 * IMG), jnp.bfloat16)
    for local in range(SBLOCK):
        lhs = rows_ref[local]
        for y in range(2):
            real = maps_ref[y, local, 0]
            imag = maps_ref[y, local, 1]
            filled = jnp.concatenate(
                [
                    jnp.concatenate([real, imag], axis=1),
                    jnp.concatenate([-imag, real], axis=1),
                ],
                axis=0,
            )
            halves = [filled, blank] if y == 0 else [blank, filled]
            mixed = jnp.dot(
                lhs, jnp.concatenate(halves, axis=0), preferred_element_type=jnp.float32
            )

            def piece(index, part):
                return mixed[
                    index * coil_share : (index + 1) * coil_share, part * IMG : (part + 1) * IMG
                ]

            out_real = piece(0, 0)
            out_imag = piece(0, 1)
            for p in range(1, KSIZE):
                cosine = waves[p - 1]
                sine = waves[KSIZE - 2 + p]
                out_real = out_real + (
                    piece(p, 0) * cosine - piece(KSIZE - 1 + p, 1) * sine
                )
                out_imag = out_imag + (
                    piece(p, 1) * cosine + piece(KSIZE - 1 + p, 0) * sine
                )
            out_ref[y, local, 0] = out_real.astype(jnp.bfloat16)
            out_ref[y, local, 1] = out_imag.astype(jnp.bfloat16)


def apply_rows(rows, maps):
    slices = rows.shape[0]
    width = maps.shape[0]
    coil_share = COILS // 2
    return pl.pallas_call(
        apply_kernel,
        grid=(slices // SBLOCK,),
        in_specs=[
            pl.BlockSpec((SBLOCK,) + rows.shape[1:], lambda i: (i, 0, 0)),
            pl.BlockSpec((width, SBLOCK, 2, COILS, IMG), lambda i: (0, i, 0, 0, 0)),
            pl.BlockSpec((16, IMG), lambda i: (0, 0)),
        ],
        out_specs=pl.BlockSpec((width, SBLOCK, 2, coil_share, IMG), lambda i: (0, i, 0, 0, 0)),
        out_shape=jax.ShapeDtypeStruct((width, slices, 2, coil_share, IMG), jnp.bfloat16),
        compiler_params=pltpu.CompilerParams(dimension_semantics=("arbitrary",)),
        name="apply_rows",
    )(rows, maps, jnp.asarray(phase_table()))


def shards(basis, picks, coil_maps):
    half = lax.axis_index("col").astype(jnp.int32).reshape(1)
    keep, send = partial_kernels(basis[0], picks)
    got = lax.ppermute(send, "col", [(0, 1), (1, 0)])
    rows = column_rows(half, keep, got)
    rows = rows.reshape(lax.axis_size("slc"), *rows.shape[2:])
    rows = lax.all_to_all(rows, "slc", split_axis=0, concat_axis=0, tiled=True)
    return apply_rows(rows, coil_maps)


def solution(mesh):
    placed = (P("slc", None, None, "col"), P("slc", "col"), P("slc", None, None, None, None))
    return jax.shard_map(
        shards,
        mesh=mesh,
        in_specs=placed,
        out_specs=P("slc", None, None, "col", None),
        check_vma=False,
    )
```

```python
import math

import jax
import jax.numpy as jnp
import numpy as np
from jax import lax
from jax.experimental import pallas as pl
from jax.experimental.pallas import tpu as pltpu
from jax.sharding import PartitionSpec as P

COILS = 32
KSIZE = 6
RANK = 608
IMG = 128
SPAN = 2 * KSIZE - 1
LANES = 128
AROWS = KSIZE * COILS
WIDE = 384
SBLOCK = 8


def gram_kernel(picks_ref, basis_ref, keep_ref, send_ref, buffer, onehot, rows, left, right, sems):
    windows = basis_ref.shape[1]
    width = basis_ref.shape[2]
    used = picks_ref.shape[1]
    cuts = [(0, 512), (512, width - 512)]
    copies = [
        pltpu.make_async_copy(
            basis_ref.at[part, :, pl.ds(first, size)],
            buffer.at[part, :, pl.ds(first, size)],
            sems.at[part, index],
        )
        for part in range(2)
        for index, (first, size) in enumerate(cuts)
    ]
    for copy in copies:
        copy.start()

    wanted = jnp.concatenate(
        [picks_ref[...], jnp.full((1, WIDE - used), -1, jnp.int32)], axis=1
    )
    wanted = jnp.broadcast_to(wanted, (LANES, WIDE)).T[:used]
    lane = lax.broadcasted_iota(jnp.int32, (used, LANES), 1)
    for first in range(0, windows, LANES):
        size = min(LANES, windows - first)
        match = jnp.where(wanted == lane + first, 1.0, 0.0).astype(jnp.bfloat16)
        onehot[:, first : first + size] = match[:, :size]
    right[:, AROWS:, :] = jnp.zeros((2, right.shape[1] - AROWS, right.shape[2]), jnp.bfloat16)

    for part in range(2):
        for index, (first, size) in enumerate(cuts):
            copies[part * len(cuts) + index].wait()
            picked = jnp.dot(
                onehot[...],
                buffer[part, :, first : first + size],
                preferred_element_type=jnp.float32,
            )
            picked = jnp.concatenate([picked, jnp.zeros((WIDE - used, size), jnp.float32)], axis=0)
            for tile in range(WIDE // LANES):
                rows[part, tile, first : first + size] = picked[
                    tile * LANES : (tile + 1) * LANES
                ].T
        for a in range(KSIZE):
            for b in range(KSIZE):
                for tile in range(WIDE // LANES):
                    block = rows[
                        part, tile, pl.ds(a * KSIZE + b, COILS, stride=KSIZE * KSIZE), :
                    ].astype(jnp.bfloat16)
                    row = slice(a * COILS, (a + 1) * COILS)
                    spot = slice(b * WIDE + tile * LANES, b * WIDE + (tile + 1) * LANES)
                    left[part, row, spot] = block
                    right[part, row, spot] = block

    def against(q, part):
        depth = (KSIZE - q) * WIDE
        lhs = left[:, :, :depth].reshape(2 * AROWS, depth)
        return lax.dot_general(
            lhs,
            right[part, :, q * WIDE :],
            (((1,), (1,)), ((), ())),
            preferred_element_type=jnp.float32,
        )

    pad = jnp.zeros((COILS, WIDE - right.shape[1]), jnp.float32)
    for q in range(KSIZE):
        with_real = against(q, 0)
        with_imag = against(q, 1)
        pair = (
            with_real[:AROWS] + with_imag[AROWS:],
            with_real[AROWS:] - with_imag[:AROWS],
        )
        for part in range(2):
            total = None
            for a in range(KSIZE):
                block = jnp.concatenate([pair[part][a * COILS : (a + 1) * COILS], pad], axis=1)
                shift = (KSIZE - 1 - a) * COILS
                moved = pltpu.roll(block, shift, 1) if shift else block
                total = moved if total is None else total + moved
            keep_ref[q, part] = total
            send_ref[q, part] = total.astype(jnp.bfloat16)


def partial_kernels(basis, picks):
    turned = pltpu.with_memory_space_constraint(jnp.transpose(basis, (0, 2, 1)), pltpu.HBM)
    parts, windows, rows = turned.shape
    used = picks.shape[1]
    return pl.pallas_call(
        gram_kernel,
        in_specs=[
            pl.BlockSpec(memory_space=pltpu.VMEM),
            pl.BlockSpec(memory_space=pltpu.HBM),
        ],
        out_specs=[pl.BlockSpec(memory_space=pltpu.VMEM)] * 2,
        out_shape=[
            jax.ShapeDtypeStruct((KSIZE, 2, COILS, WIDE), jnp.float32),
            jax.ShapeDtypeStruct((KSIZE, 2, COILS, WIDE), jnp.bfloat16),
        ],
        scratch_shapes=[
            pltpu.VMEM((parts, windows, rows), jnp.bfloat16),
            pltpu.VMEM((used, windows), jnp.bfloat16),
            pltpu.VMEM((parts, WIDE // LANES, rows, LANES), jnp.float32),
            pltpu.VMEM((2, AROWS, KSIZE * WIDE), jnp.bfloat16),
            pltpu.VMEM((2, 256, KSIZE * WIDE), jnp.bfloat16),
            pltpu.SemaphoreType.DMA((parts, 2)),
        ],
        compiler_params=pltpu.CompilerParams(vmem_limit_bytes=24 * 2**20),
        name="partial_kernels",
    )(picks, turned)


def transform_table():
    half = IMG // 4
    table = np.zeros((half, 16, LANES), np.float32)
    for first in range(half):
        for q in range(1, KSIZE):
            lanes_y = np.repeat(2 * first + np.arange(2), LANES // 2)
            angle = 2.0 * math.pi * ((q * lanes_y) % IMG) / IMG
            table[first, q - 1] = np.cos(angle)
            table[first, KSIZE - 2 + q] = np.sin(angle)
    return table


def transform_kernel(half_ref, keep_ref, got_ref, table_ref, out_ref, whole, turned, terms):
    coil_share = COILS // 2

    def build():
        factor = 1.0 / (2.0 * RANK * KSIZE * KSIZE)
        own = pl.multiple_of(half_ref[0] * coil_share, coil_share)
        lane = lax.broadcasted_iota(jnp.int32, (coil_share, LANES), 1)
        group = lane // COILS
        even_slot = group % 2 == 0
        low_half = lane < LANES // 2
        swap_sign = jnp.where(even_slot, -1.0, 1.0)
        centre = KSIZE - 1

        def forward(q):
            found = []
            for tile in range(WIDE // LANES):
                lanes = slice(tile * LANES, (tile + 1) * LANES)
                real = whole[q, 0, pl.ds(own, coil_share), lanes]
                imag = whole[q, 1, pl.ds(own, coil_share), lanes]
                first = jnp.where(even_slot, real, pltpu.roll(imag, COILS, 1))
                second = jnp.where(even_slot, pltpu.roll(real, LANES - COILS, 1), imag)
                first_turned = pltpu.roll(first, LANES // 2, 1)
                second_turned = pltpu.roll(second, LANES // 2, 1)
                found += [
                    jnp.where(low_half, first, first_turned),
                    jnp.where(low_half, second, second_turned),
                    jnp.where(low_half, first_turned, first),
                    jnp.where(low_half, second_turned, second),
                ]
            return found[:SPAN]

        def place(index, values):
            terms[index, :coil_share] = values[centre]
            for offset in range(1, KSIZE):
                upper = values[centre + offset]
                lower = values[centre - offset]
                even = offset * coil_share
                odd = (offset + KSIZE - 1) * coil_share
                terms[index, even : even + coil_share] = upper + lower
                terms[index, odd : odd + coil_share] = upper - lower

        def one_shift(q, carry):
            real = (keep_ref[q, 0] + got_ref[q, 0].astype(jnp.float32)) * factor
            imag = (keep_ref[q, 1] + got_ref[q, 1].astype(jnp.float32)) * factor
            whole[q, 0] = real
            whole[q, 1] = imag
            turned[...] = jnp.concatenate([real, -imag, real, -imag], axis=0).T
            ahead = forward(q)
            sums = []
            gaps = []
            for p in range(SPAN):
                row = pl.multiple_of((SPAN - 1 - p) * COILS + own, coil_share)
                behind = turned[pl.ds(row, coil_share), :]
                sums.append(ahead[p] + behind)
                gaps.append(pltpu.roll(ahead[p] - behind, COILS, 1) * swap_sign)
            place(q, sums)
            place(KSIZE - 1 + q, gaps)
            return carry

        for part in range(2):
            whole[0, part] = (keep_ref[0, part] + got_ref[0, part].astype(jnp.float32)) * factor
        place(0, forward(0))
        lax.fori_loop(1, KSIZE, one_shift, 0)

    build()
    blocks = table_ref.shape[0]
    group_size = 2

    def one(step, carry):
        places = [step * group_size + extra for extra in range(group_size)]
        weights = [
            [
                jnp.broadcast_to(table_ref[place, index : index + 1, :], (8, LANES))
                for index in range(2 * KSIZE - 2)
            ]
            for place in places
        ]
        for block in range(SPAN):
            made = [[] for _ in places]
            for sub in range(2):
                rows = slice(block * coil_share + sub * 8, block * coil_share + sub * 8 + 8)
                cells = [terms[index, rows] for index in range(2 * KSIZE - 1)]
                for extra in range(group_size):
                    even = cells[0]
                    odd = None
                    for q in range(1, KSIZE):
                        piece = (
                            cells[q] * weights[extra][q - 1]
                            + cells[KSIZE - 1 + q] * weights[extra][KSIZE - 2 + q]
                        )
                        if q % 2 == 0:
                            even = even + piece
                        else:
                            odd = piece if odd is None else odd + piece
                    made[extra].append((even + odd, even - odd))
            rows = slice(block * coil_share, (block + 1) * coil_share)
            for extra, place in enumerate(places):
                for sign in range(2):
                    whole_rows = jnp.concatenate([half[sign] for half in made[extra]], axis=0)
                    out_ref[place + sign * blocks, rows, :] = whole_rows.astype(jnp.bfloat16)
        return carry

    lax.fori_loop(0, blocks // group_size, one, 0)


def column_rows(half, keep, got):
    blocks = IMG // 2
    rows = SPAN * COILS // 2
    return pl.pallas_call(
        transform_kernel,
        in_specs=[pl.BlockSpec(memory_space=pltpu.SMEM)]
        + [pl.BlockSpec(memory_space=pltpu.VMEM)] * 3,
        out_specs=pl.BlockSpec(memory_space=pltpu.VMEM),
        scratch_shapes=[
            pltpu.VMEM((KSIZE, 2, COILS, WIDE), jnp.float32),
            pltpu.VMEM((WIDE, LANES), jnp.float32),
            pltpu.VMEM((2 * KSIZE - 1, rows + 8, LANES), jnp.float32),
        ],
        out_shape=jax.ShapeDtypeStruct((blocks, rows, LANES), jnp.bfloat16),
        compiler_params=pltpu.CompilerParams(vmem_limit_bytes=16 * 2**20),
        name="column_rows",
    )(half, keep, got, jnp.asarray(transform_table()))


def phase_table():
    table = np.zeros((16, IMG), np.float32)
    for p in range(1, KSIZE):
        angle = 2.0 * math.pi * ((p * np.arange(IMG)) % IMG) / IMG
        table[p - 1] = np.cos(angle)
        table[KSIZE - 2 + p] = np.sin(angle)
    return table


def apply_kernel(rows_ref, maps_ref, table_ref, out_ref, result, sems):
    coil_share = COILS // 2
    slices = rows_ref.shape[0]
    waves = [
        jnp.broadcast_to(table_ref[index : index + 1, :], (coil_share, IMG))
        for index in range(2 * KSIZE - 2)
    ]
    blank = jnp.zeros((2 * COILS, 2 * IMG), jnp.bfloat16)

    def one(index, y):
        real = maps_ref[y, index, 0]
        imag = maps_ref[y, index, 1]
        filled = jnp.concatenate(
            [
                jnp.concatenate([real, imag], axis=1),
                jnp.concatenate([-imag, real], axis=1),
            ],
            axis=0,
        )
        halves = [filled, blank] if y == 0 else [blank, filled]
        mixed = jnp.dot(
            rows_ref[index], jnp.concatenate(halves, axis=0), preferred_element_type=jnp.float32
        )

        def piece(place, part):
            return mixed[
                place * coil_share : (place + 1) * coil_share, part * IMG : (part + 1) * IMG
            ]

        out_real = piece(0, 0)
        out_imag = piece(0, 1)
        for p in range(1, KSIZE):
            cosine = waves[p - 1]
            sine = waves[KSIZE - 2 + p]
            out_real = out_real + (piece(p, 0) * cosine - piece(KSIZE - 1 + p, 1) * sine)
            out_imag = out_imag + (piece(p, 1) * cosine + piece(KSIZE - 1 + p, 0) * sine)
        result[y, index, 0] = out_real.astype(jnp.bfloat16)
        result[y, index, 1] = out_imag.astype(jnp.bfloat16)

    def write(step, y):
        span = pl.ds(step * SBLOCK, SBLOCK)
        return pltpu.make_async_copy(result.at[y, span], out_ref.at[y, span], sems.at[step, y])

    def block(step, carry):
        for local in range(SBLOCK):
            for y in range(2):
                one(step * SBLOCK + local, y)
        for y in range(2):
            write(step, y).start()
        return carry

    steps = slices // SBLOCK
    lax.fori_loop(0, steps, block, 0)

    def finish(step, carry):
        for y in range(2):
            write(step, y).wait()
        return carry

    lax.fori_loop(0, steps, finish, 0)


def apply_rows(rows, maps):
    slices = rows.shape[0]
    width = maps.shape[0]
    shape = (width, slices, 2, COILS // 2, IMG)
    return pl.pallas_call(
        apply_kernel,
        in_specs=[pl.BlockSpec(memory_space=pltpu.VMEM)] * 3,
        out_specs=pl.BlockSpec(memory_space=pltpu.HBM),
        out_shape=jax.ShapeDtypeStruct(shape, jnp.bfloat16),
        scratch_shapes=[
            pltpu.VMEM(shape, jnp.bfloat16),
            pltpu.SemaphoreType.DMA((slices // SBLOCK, width)),
        ],
        compiler_params=pltpu.CompilerParams(vmem_limit_bytes=16 * 2**20),
        name="apply_rows",
    )(rows, maps, jnp.asarray(phase_table()))


def shards(basis, picks, coil_maps):
    half = lax.axis_index("col").astype(jnp.int32).reshape(1)
    keep, send = partial_kernels(basis[0], picks)
    got = lax.ppermute(send, "col", [(0, 1), (1, 0)])
    rows = column_rows(half, keep, got)
    rows = lax.all_to_all(rows, "slc", split_axis=0, concat_axis=0, tiled=True)
    return apply_rows(rows, coil_maps)


def solution(mesh):
    placed = (P("slc", None, None, "col"), P("slc", "col"), P("slc", None, None, None, None))
    return jax.shard_map(
        shards,
        mesh=mesh,
        in_specs=placed,
        out_specs=P("slc", None, None, "col", None),
        check_vma=False,
    )
```

```python
import math

import jax
import jax.numpy as jnp
import numpy as np
from jax import lax
from jax.experimental import pallas as pl
from jax.experimental.pallas import tpu as pltpu
from jax.sharding import PartitionSpec as P

COILS = 32
KSIZE = 6
RANK = 608
IMG = 128
SPAN = 2 * KSIZE - 1
LANES = 128
AROWS = KSIZE * COILS
WIDE = 384
SBLOCK = 4
PACKED = 136
BF = jnp.bfloat16


def gram_kernel(picks_ref, basis_ref, keep_ref, send_ref, buffer, onehot, rows, left, right, sems):
    windows = basis_ref.shape[1]
    width = basis_ref.shape[2]
    used = picks_ref.shape[1]
    cuts = [(0, 512), (512, width - 512)]
    copies = [
        pltpu.make_async_copy(
            basis_ref.at[part, :, pl.ds(first, size)],
            buffer.at[part, :, pl.ds(first, size)],
            sems.at[part, index],
        )
        for part in range(2)
        for index, (first, size) in enumerate(cuts)
    ]
    for copy in copies:
        copy.start()

    wanted = jnp.concatenate(
        [picks_ref[...], jnp.full((1, WIDE - used), -1, jnp.int32)], axis=1
    )
    wanted = jnp.broadcast_to(wanted, (LANES, WIDE)).T[:used]
    lane = lax.broadcasted_iota(jnp.int32, (used, LANES), 1)
    for first in range(0, windows, LANES):
        size = min(LANES, windows - first)
        match = jnp.where(wanted == lane + first, 1.0, 0.0).astype(jnp.bfloat16)
        onehot[:, first : first + size] = match[:, :size]
    right[:, AROWS:, :] = jnp.zeros((2, right.shape[1] - AROWS, right.shape[2]), jnp.bfloat16)

    for part in range(2):
        for index, (first, size) in enumerate(cuts):
            copies[part * len(cuts) + index].wait()
            picked = jnp.dot(
                onehot[...],
                buffer[part, :, first : first + size],
                preferred_element_type=jnp.float32,
            )
            picked = jnp.concatenate([picked, jnp.zeros((WIDE - used, size), jnp.float32)], axis=0)
            for tile in range(WIDE // LANES):
                rows[part, tile, first : first + size] = picked[
                    tile * LANES : (tile + 1) * LANES
                ].T
        for a in range(KSIZE):
            for b in range(KSIZE):
                for tile in range(WIDE // LANES):
                    block = rows[
                        part, tile, pl.ds(a * KSIZE + b, COILS, stride=KSIZE * KSIZE), :
                    ].astype(jnp.bfloat16)
                    row = slice(a * COILS, (a + 1) * COILS)
                    spot = slice(b * WIDE + tile * LANES, b * WIDE + (tile + 1) * LANES)
                    left[part, row, spot] = block
                    right[part, row, spot] = block

    def against(q, part):
        depth = (KSIZE - q) * WIDE
        lhs = left[:, :, :depth].reshape(2 * AROWS, depth)
        return lax.dot_general(
            lhs,
            right[part, :, q * WIDE :],
            (((1,), (1,)), ((), ())),
            preferred_element_type=jnp.float32,
        )

    pad = jnp.zeros((COILS, WIDE - right.shape[1]), jnp.float32)
    for q in range(KSIZE):
        with_real = against(q, 0)
        with_imag = against(q, 1)
        pair = (
            with_real[:AROWS] + with_imag[AROWS:],
            with_real[AROWS:] - with_imag[:AROWS],
        )
        for part in range(2):
            total = None
            for a in range(KSIZE):
                block = jnp.concatenate([pair[part][a * COILS : (a + 1) * COILS], pad], axis=1)
                shift = (KSIZE - 1 - a) * COILS
                moved = pltpu.roll(block, shift, 1) if shift else block
                total = moved if total is None else total + moved
            keep_ref[q, part] = total
            send_ref[q, part] = total.astype(jnp.bfloat16)


def partial_kernels(basis, picks):
    turned = pltpu.with_memory_space_constraint(jnp.transpose(basis, (0, 2, 1)), pltpu.HBM)
    parts, windows, rows = turned.shape
    used = picks.shape[1]
    return pl.pallas_call(
        gram_kernel,
        in_specs=[
            pl.BlockSpec(memory_space=pltpu.VMEM),
            pl.BlockSpec(memory_space=pltpu.HBM),
        ],
        out_specs=[pl.BlockSpec(memory_space=pltpu.VMEM)] * 2,
        out_shape=[
            jax.ShapeDtypeStruct((KSIZE, 2, COILS, WIDE), jnp.float32),
            jax.ShapeDtypeStruct((KSIZE, 2, COILS, WIDE), jnp.bfloat16),
        ],
        scratch_shapes=[
            pltpu.VMEM((parts, windows, rows), jnp.bfloat16),
            pltpu.VMEM((used, windows), jnp.bfloat16),
            pltpu.VMEM((parts, WIDE // LANES, rows, LANES), jnp.float32),
            pltpu.VMEM((2, AROWS, KSIZE * WIDE), jnp.bfloat16),
            pltpu.VMEM((2, 256, KSIZE * WIDE), jnp.bfloat16),
            pltpu.SemaphoreType.DMA((parts, 2)),
        ],
        compiler_params=pltpu.CompilerParams(vmem_limit_bytes=24 * 2**20),
        name="partial_kernels",
    )(picks, turned)


def transform_table():
    half = IMG // 4
    table = np.zeros((half, 16, LANES), np.float32)
    for first in range(half):
        for q in range(1, KSIZE):
            lanes_y = np.repeat(2 * first + np.arange(2), LANES // 2)
            angle = 2.0 * math.pi * ((q * lanes_y) % IMG) / IMG
            table[first, q - 1] = np.cos(angle)
            table[first, KSIZE - 2 + q] = np.sin(angle)
    return table


def transform_kernel(half_ref, keep_ref, got_ref, table_ref, out_ref, whole, turned, terms):
    coil_share = COILS // 2

    def build():
        factor = 1.0 / (2.0 * RANK * KSIZE * KSIZE)
        own = pl.multiple_of(half_ref[0] * coil_share, coil_share)
        other = pl.multiple_of(coil_share - half_ref[0] * coil_share, coil_share)
        lane = lax.broadcasted_iota(jnp.int32, (coil_share, LANES), 1)
        group = lane // COILS
        even_slot = group % 2 == 0
        low_half = lane < LANES // 2
        swap_sign = jnp.where(even_slot, -1.0, 1.0)
        centre = KSIZE - 1

        own_lane = lane // coil_share % 2 == 0
        upper_half = half_ref[0] == 1

        def own_first(value):
            down = pltpu.roll(value, LANES - coil_share, 1)
            up = pltpu.roll(value, coil_share, 1)
            return jnp.where(upper_half, jnp.where(own_lane, down, up), value)

        def forward(q):
            found = []
            for tile in range(WIDE // LANES):
                lanes = slice(tile * LANES, (tile + 1) * LANES)
                real = own_first(whole[q, 0, pl.ds(own, coil_share), lanes])
                imag = own_first(whole[q, 1, pl.ds(own, coil_share), lanes])
                first = jnp.where(even_slot, real, pltpu.roll(imag, COILS, 1))
                second = jnp.where(even_slot, pltpu.roll(real, LANES - COILS, 1), imag)
                first_turned = pltpu.roll(first, LANES // 2, 1)
                second_turned = pltpu.roll(second, LANES // 2, 1)
                found += [
                    jnp.where(low_half, first, first_turned),
                    jnp.where(low_half, second, second_turned),
                    jnp.where(low_half, first_turned, first),
                    jnp.where(low_half, second_turned, second),
                ]
            return found[:SPAN]

        toward_own = LANES - coil_share

        def place(index, values):
            terms[index, :coil_share] = values[centre]
            gaps = []
            for offset in range(1, KSIZE):
                upper = values[centre + offset]
                lower = values[centre - offset]
                row = offset * coil_share
                terms[index, row : row + coil_share] = jnp.where(own_lane, upper, upper + lower)
                gaps.append(upper - lower)
            row = KSIZE * coil_share
            for pair in range(2):
                moved = pltpu.roll(gaps[2 * pair + 1], toward_own, 1)
                terms[index, row : row + coil_share] = jnp.where(own_lane, moved, gaps[2 * pair])
                row += coil_share
            moved = pltpu.roll(gaps[4], toward_own, 1)
            rest = coil_share // 2
            terms[index, row : row + rest] = jnp.where(own_lane[:rest], moved[rest:], gaps[4][:rest])

        def one_shift(q, carry):
            real = (keep_ref[q, 0] + got_ref[q, 0].astype(jnp.float32)) * factor
            imag = (keep_ref[q, 1] + got_ref[q, 1].astype(jnp.float32)) * factor
            whole[q, 0] = real
            whole[q, 1] = imag
            ordered = [
                whole[q, part, pl.ds(first, coil_share), :]
                for part in range(2)
                for first in (own, other)
            ]
            ordered = [ordered[0], ordered[1], -ordered[2], -ordered[3]]
            turned[...] = jnp.concatenate(ordered + ordered, axis=0).T
            ahead = forward(q)
            sums = []
            gaps = []
            for p in range(SPAN):
                row = pl.multiple_of((SPAN - 1 - p) * COILS + own, coil_share)
                behind = turned[pl.ds(row, coil_share), :]
                sums.append(ahead[p] + behind)
                gaps.append(pltpu.roll(ahead[p] - behind, COILS, 1) * swap_sign)
            place(q, sums)
            place(KSIZE - 1 + q, gaps)
            return carry

        for part in range(2):
            whole[0, part] = (keep_ref[0, part] + got_ref[0, part].astype(jnp.float32)) * factor
        place(0, forward(0))
        lax.fori_loop(1, KSIZE, one_shift, 0)

    build()
    blocks = table_ref.shape[0]
    group_size = 2

    def one(step, carry):
        places = [step * group_size + extra for extra in range(group_size)]
        weights = [
            [
                jnp.broadcast_to(table_ref[place, index : index + 1, :], (8, LANES))
                for index in range(2 * KSIZE - 2)
            ]
            for place in places
        ]
        for first in range(0, PACKED, coil_share):
            made = [[] for _ in places]
            last = min(first + coil_share, PACKED)
            for row in range(first, last, 8):
                cells = [terms[index, row : row + 8] for index in range(2 * KSIZE - 1)]
                for extra in range(group_size):
                    even = cells[0]
                    odd = None
                    for q in range(1, KSIZE):
                        piece = (
                            cells[q] * weights[extra][q - 1]
                            + cells[KSIZE - 1 + q] * weights[extra][KSIZE - 2 + q]
                        )
                        if q % 2 == 0:
                            even = even + piece
                        else:
                            odd = piece if odd is None else odd + piece
                    made[extra].append((even + odd, even - odd))
            for extra, place in enumerate(places):
                for sign in range(2):
                    whole_rows = jnp.concatenate([half[sign] for half in made[extra]], axis=0)
                    out_ref[place + sign * blocks, first:last, :] = whole_rows.astype(jnp.bfloat16)
        return carry

    lax.fori_loop(0, blocks // group_size, one, 0)


def column_rows(half, keep, got):
    blocks = IMG // 2
    return pl.pallas_call(
        transform_kernel,
        in_specs=[pl.BlockSpec(memory_space=pltpu.SMEM)]
        + [pl.BlockSpec(memory_space=pltpu.VMEM)] * 3,
        out_specs=pl.BlockSpec(memory_space=pltpu.VMEM),
        scratch_shapes=[
            pltpu.VMEM((KSIZE, 2, COILS, WIDE), jnp.float32),
            pltpu.VMEM((WIDE, LANES), jnp.float32),
            pltpu.VMEM((2 * KSIZE - 1, PACKED, LANES), jnp.float32),
        ],
        out_shape=jax.ShapeDtypeStruct((blocks, PACKED, LANES), jnp.bfloat16),
        compiler_params=pltpu.CompilerParams(vmem_limit_bytes=16 * 2**20),
        name="column_rows",
    )(half, keep, got, jnp.asarray(transform_table()))


def phase_table():
    table = np.zeros((16, IMG), np.float32)
    for p in range(1, KSIZE):
        angle = 2.0 * math.pi * ((p * np.arange(IMG)) % IMG) / IMG
        table[p - 1] = np.cos(angle)
        table[KSIZE - 2 + p] = np.sin(angle)
    return table


def apply_kernel(half_ref, rows_ref, maps_ref, table_ref, out_ref, result, even_rows, odd_rows, sems):
    coil_share = COILS // 2
    slices = rows_ref.shape[0]
    waves = [
        jnp.broadcast_to(table_ref[index : index + 1, :], (coil_share, IMG))
        for index in range(2 * KSIZE - 2)
    ]
    blank = jnp.zeros((2 * COILS, 2 * IMG), jnp.bfloat16)
    own = pl.multiple_of(half_ref[0] * coil_share, coil_share)
    other = pl.multiple_of(coil_share - half_ref[0] * coil_share, coil_share)
    lane = lax.broadcasted_iota(jnp.int32, (coil_share, LANES), 1)
    own_lane = lane // coil_share % 2 == 0
    group = lane // COILS
    groups = LANES // COILS
    buffers = (even_rows, odd_rows)

    def unpack(index, lhs, local):
        def tile(place):
            return rows_ref[index, place * coil_share : (place + 1) * coil_share, :]

        def spread(packed):
            return packed, pltpu.roll(packed, coil_share, 1)

        first, second = spread(tile(KSIZE))
        third, fourth = spread(tile(KSIZE + 1))
        tail = spread(rows_ref[index, (KSIZE + 2) * coil_share :, :])
        crossed = [first, second, third, fourth, jnp.concatenate(tail, axis=0)]
        merged = [tile(place) for place in range(KSIZE)]
        stacked = jnp.concatenate(merged[1:] + [jnp.zeros((3 * coil_share, LANES), BF)], axis=0).T
        strips = []
        for target in range(groups):
            strip = stacked[target * COILS : target * COILS + coil_share]
            strips.append(-strip if target % 2 else strip)
        lhs[local, :coil_share] = merged[0]
        for p in range(1, KSIZE):
            mirror = None
            for target in range(groups):
                shift = (target * COILS - (p - 1) * coil_share) % LANES
                moved = pltpu.roll(strips[target], shift, 1) if shift else strips[target]
                mirror = moved if mirror is None else jnp.where(group == target, moved, mirror)
            row = p * coil_share
            lhs[local, row : row + coil_share] = jnp.where(
                own_lane, merged[p] + mirror, merged[p]
            )
            row = (p + KSIZE - 1) * coil_share
            lhs[local, row : row + coil_share] = jnp.where(
                own_lane, merged[p] - mirror, crossed[p - 1]
            )

    def one(index, y, lhs, local):
        real, imag = [
            jnp.concatenate(
                [maps_ref[y, index, part, pl.ds(first, coil_share)] for first in (own, other)],
                axis=0,
            )
            for part in range(2)
        ]
        filled = jnp.concatenate(
            [
                jnp.concatenate([real, imag], axis=1),
                jnp.concatenate([-imag, real], axis=1),
            ],
            axis=0,
        )
        halves = [filled, blank] if y == 0 else [blank, filled]
        mixed = jnp.dot(
            lhs[local], jnp.concatenate(halves, axis=0), preferred_element_type=jnp.float32
        )

        def piece(place, part):
            return mixed[
                place * coil_share : (place + 1) * coil_share, part * IMG : (part + 1) * IMG
            ]

        out_real = piece(0, 0)
        out_imag = piece(0, 1)
        for p in range(1, KSIZE):
            cosine = waves[p - 1]
            sine = waves[KSIZE - 2 + p]
            out_real = out_real + (piece(p, 0) * cosine - piece(KSIZE - 1 + p, 1) * sine)
            out_imag = out_imag + (piece(p, 1) * cosine + piece(KSIZE - 1 + p, 0) * sine)
        result[y, index, 0] = out_real.astype(jnp.bfloat16)
        result[y, index, 1] = out_imag.astype(jnp.bfloat16)

    def write(step):
        span = pl.ds(step * 2 * SBLOCK, 2 * SBLOCK)
        return pltpu.make_async_copy(result.at[:, span], out_ref.at[:, span], sems.at[step])

    def block(step, carry):
        first = step * 2 * SBLOCK
        for current, following in ((0, 1), (1, 0)):
            for local in range(SBLOCK):
                index = first + current * SBLOCK + local
                ahead = jnp.minimum(index + SBLOCK, slices - 1)
                unpack(ahead, buffers[following], local)
                for y in range(2):
                    one(index, y, buffers[current], local)
        write(step).start()
        return carry

    steps = slices // (2 * SBLOCK)
    for local in range(SBLOCK):
        unpack(local, buffers[0], local)
    lax.fori_loop(0, steps, block, 0)
    for step in range(steps):
        write(step).wait()


def apply_rows(half, rows, maps):
    slices = rows.shape[0]
    width = maps.shape[0]
    shape = (width, slices, 2, COILS // 2, IMG)
    return pl.pallas_call(
        apply_kernel,
        in_specs=[pl.BlockSpec(memory_space=pltpu.SMEM)]
        + [pl.BlockSpec(memory_space=pltpu.VMEM)] * 3,
        out_specs=pl.BlockSpec(memory_space=pltpu.HBM),
        out_shape=jax.ShapeDtypeStruct(shape, jnp.bfloat16),
        scratch_shapes=[
            pltpu.VMEM(shape, jnp.bfloat16),
            pltpu.VMEM((SBLOCK, SPAN * COILS // 2, LANES), jnp.bfloat16),
            pltpu.VMEM((SBLOCK, SPAN * COILS // 2, LANES), jnp.bfloat16),
            pltpu.SemaphoreType.DMA((slices // (2 * SBLOCK),)),
        ],
        compiler_params=pltpu.CompilerParams(vmem_limit_bytes=16 * 2**20),
        name="apply_rows",
    )(half, rows, maps, jnp.asarray(phase_table()))


def shards(basis, picks, coil_maps):
    half = lax.axis_index("col").astype(jnp.int32).reshape(1)
    keep, send = partial_kernels(basis[0], picks)
    got = lax.ppermute(send, "col", [(0, 1), (1, 0)])
    rows = column_rows(half, keep, got)
    rows = lax.all_to_all(rows, "slc", split_axis=0, concat_axis=0, tiled=True)
    return apply_rows(half, rows, coil_maps)


def solution(mesh):
    placed = (P("slc", None, None, "col"), P("slc", "col"), P("slc", None, None, None, None))
    return jax.shard_map(
        shards,
        mesh=mesh,
        in_specs=placed,
        out_specs=P("slc", None, None, "col", None),
        check_vma=False,
    )
```

```python
import math

import jax
import jax.numpy as jnp
import numpy as np
from jax import lax
from jax.experimental import pallas as pl
from jax.experimental.pallas import tpu as pltpu
from jax.sharding import PartitionSpec as P

COILS = 32
KSIZE = 6
RANK = 608
IMG = 128
SPAN = 2 * KSIZE - 1
LANES = 128
AROWS = KSIZE * COILS
WIDE = 384
SBLOCK = 16
PACKED = 136
DEPTH = 2
BF = jnp.bfloat16


def gram_kernel(
    half_ref, picks_ref, basis_ref, keep_ref, send_ref,
    chosen, buffer, onehot, picked, rows, left, right, pairs, sems, pick_sem,
):
    windows = basis_ref.shape[1]
    width = basis_ref.shape[2]
    used = picks_ref.shape[1]
    coil_share = COILS // 2
    own = pl.multiple_of(half_ref[0] * coil_share, coil_share)
    other = pl.multiple_of(coil_share - half_ref[0] * coil_share, coil_share)
    cuts = [(0, 256), (256, 384), (640, width - 640)]
    fetch = pltpu.make_async_copy(picks_ref, chosen, pick_sem.at[0])
    fetch.start()
    copies = [
        pltpu.make_async_copy(
            basis_ref.at[part, :, pl.ds(first, size)],
            buffer.at[part, :, pl.ds(first, size)],
            sems.at[part, index],
        )
        for part in range(2)
        for index, (first, size) in enumerate(cuts)
    ]
    for copy in copies[:DEPTH]:
        copy.start()

    right[:, AROWS:, :] = jnp.zeros((2, right.shape[1] - AROWS, right.shape[2]), jnp.bfloat16)
    for slot in range(2):
        picked[slot, used:] = jnp.zeros((WIDE - used, picked.shape[2]), jnp.float32)
    fetch.wait()
    wanted = jnp.concatenate([chosen[...], jnp.full((1, WIDE - used), -1, jnp.int32)], axis=1)
    wanted = jnp.broadcast_to(wanted, (LANES, WIDE)).T[:used]
    lane = lax.broadcasted_iota(jnp.int32, (used, LANES), 1)
    for first in range(0, windows, LANES):
        size = min(LANES, windows - first)
        match = jnp.where(wanted == lane + first, 1.0, 0.0).astype(jnp.bfloat16)
        onehot[:, first : first + size] = match[:, :size]

    def spread(position):
        part, index = divmod(position, len(cuts))
        first, size = cuts[index]
        for tile in range(WIDE // LANES):
            rows[part, tile, first : first + size] = picked[
                position % 2, tile * LANES : (tile + 1) * LANES, :size
            ].T
        if index + 1 < len(cuts):
            return
        for a in range(KSIZE):
            for b in range(KSIZE):
                for tile in range(WIDE // LANES):
                    block = rows[
                        part, tile, pl.ds(a * KSIZE + b, COILS, stride=KSIZE * KSIZE), :
                    ].astype(jnp.bfloat16)
                    row = slice(a * COILS, (a + 1) * COILS)
                    spot = slice(b * WIDE + tile * LANES, b * WIDE + (tile + 1) * LANES)
                    left[part, row, spot] = block
                    right[part, row, spot] = block

    for position, copy in enumerate(copies):
        part, index = divmod(position, len(cuts))
        first, size = cuts[index]
        copy.wait()
        if position + DEPTH < len(copies):
            copies[position + DEPTH].start()
        picked[position % 2, :used, :size] = jnp.dot(
            onehot[...],
            buffer[part, :, first : first + size],
            preferred_element_type=jnp.float32,
        )
        if position:
            spread(position - 1)
    spread(len(copies) - 1)

    def against(q, part):
        depth = (KSIZE - q) * WIDE
        lhs = left[:, :, :depth].reshape(2 * AROWS, depth)
        return lax.dot_general(
            lhs,
            right[part, :, q * WIDE :],
            (((1,), (1,)), ((), ())),
            preferred_element_type=jnp.float32,
        )

    pad = jnp.zeros((COILS, WIDE - right.shape[1]), jnp.float32)

    def shift_sums(q):
        for part in range(2):
            total = None
            for a in range(KSIZE):
                block = pairs[q % 2, part, a * COILS : (a + 1) * COILS]
                block = jnp.concatenate([block, pad], axis=1)
                shift = (KSIZE - 1 - a) * COILS
                moved = pltpu.roll(block, shift, 1) if shift else block
                total = moved if total is None else total + moved
            keep_ref[q, part] = total
            send_ref[q, part] = keep_ref[q, part, pl.ds(other, coil_share)].astype(jnp.bfloat16)

    for q in range(KSIZE):
        with_real = against(q, 0)
        with_imag = against(q, 1)
        pairs[q % 2, 0] = with_real[:AROWS] + with_imag[AROWS:]
        pairs[q % 2, 1] = with_real[AROWS:] - with_imag[:AROWS]
        if q:
            shift_sums(q - 1)
    shift_sums(KSIZE - 1)
    lane = lax.broadcasted_iota(jnp.int32, (coil_share, WIDE), 1)
    theirs = lane // coil_share % 2 == 1 - half_ref[0]
    toward = jnp.where(half_ref[0] == 0, WIDE - coil_share, coil_share)
    for q in range(1, KSIZE, 2):
        for part in range(2):
            mixed = keep_ref[q, part, pl.ds(own, coil_share)]
            if q + 1 < KSIZE:
                extra = pltpu.roll(keep_ref[q + 1, part, pl.ds(own, coil_share)], toward, 1)
                mixed = jnp.where(theirs, mixed, extra)
            send_ref[KSIZE + q // 2, part] = mixed.astype(jnp.bfloat16)


def partial_kernels(half, basis, picks):
    turned = pltpu.with_memory_space_constraint(jnp.transpose(basis, (0, 2, 1)), pltpu.HBM)
    picks = pltpu.with_memory_space_constraint(picks, pltpu.HBM)
    parts, windows, rows = turned.shape
    used = picks.shape[1]
    return pl.pallas_call(
        gram_kernel,
        in_specs=[pl.BlockSpec(memory_space=pltpu.SMEM)]
        + [pl.BlockSpec(memory_space=pltpu.HBM)] * 2,
        out_specs=[pl.BlockSpec(memory_space=pltpu.VMEM)] * 2,
        out_shape=[
            jax.ShapeDtypeStruct((KSIZE, 2, COILS, WIDE), jnp.float32),
            jax.ShapeDtypeStruct((KSIZE + KSIZE // 2, 2, COILS // 2, WIDE), jnp.bfloat16),
        ],
        scratch_shapes=[
            pltpu.VMEM((1, used), jnp.int32),
            pltpu.VMEM((parts, windows, rows), jnp.bfloat16),
            pltpu.VMEM((used, windows), jnp.bfloat16),
            pltpu.VMEM((2, WIDE, 512), jnp.float32),
            pltpu.VMEM((parts, WIDE // LANES, rows, LANES), jnp.float32),
            pltpu.VMEM((2, AROWS, KSIZE * WIDE), jnp.bfloat16),
            pltpu.VMEM((2, 256, KSIZE * WIDE), jnp.bfloat16),
            pltpu.VMEM((2, 2, AROWS, 256), jnp.float32),
            pltpu.SemaphoreType.DMA((parts, 3)),
            pltpu.SemaphoreType.DMA((1,)),
        ],
        compiler_params=pltpu.CompilerParams(vmem_limit_bytes=28 * 2**20),
        name="partial_kernels",
    )(half, picks, turned)


def transform_table():
    half = IMG // 4
    table = np.zeros((half, 16, LANES), np.float32)
    for first in range(half):
        for q in range(1, KSIZE):
            lanes_y = np.repeat(2 * first + np.arange(2), LANES // 2)
            angle = 2.0 * math.pi * ((q * lanes_y) % IMG) / IMG
            table[first, q - 1] = np.cos(angle)
            table[first, KSIZE - 2 + q] = np.sin(angle)
    return table


def transform_kernel(half_ref, keep_ref, got_ref, table_ref, out_ref, whole, turned, terms):
    coil_share = COILS // 2

    def build():
        factor = 1.0 / (2.0 * RANK * KSIZE * KSIZE)
        own = pl.multiple_of(half_ref[0] * coil_share, coil_share)
        other = pl.multiple_of(coil_share - half_ref[0] * coil_share, coil_share)
        lane = lax.broadcasted_iota(jnp.int32, (coil_share, LANES), 1)
        group = lane // COILS
        even_slot = group % 2 == 0
        low_half = lane < LANES // 2
        swap_sign = jnp.where(even_slot, -1.0, 1.0)
        centre = KSIZE - 1

        own_lane = lane // coil_share % 2 == 0
        upper_half = half_ref[0] == 1

        def own_first(value):
            down = pltpu.roll(value, LANES - coil_share, 1)
            up = pltpu.roll(value, coil_share, 1)
            return jnp.where(upper_half, jnp.where(own_lane, down, up), value)

        def forward(q):
            found = []
            for tile in range(WIDE // LANES):
                lanes = slice(tile * LANES, (tile + 1) * LANES)
                real = own_first(whole[q, 0, :, lanes])
                imag = own_first(whole[q, 1, :, lanes])
                first = jnp.where(even_slot, real, pltpu.roll(imag, COILS, 1))
                second = jnp.where(even_slot, pltpu.roll(real, LANES - COILS, 1), imag)
                first_turned = pltpu.roll(first, LANES // 2, 1)
                second_turned = pltpu.roll(second, LANES // 2, 1)
                found += [
                    jnp.where(low_half, first, first_turned),
                    jnp.where(low_half, second, second_turned),
                    jnp.where(low_half, first_turned, first),
                    jnp.where(low_half, second_turned, second),
                ]
            return found[:SPAN]

        toward_own = LANES - coil_share

        def place(index, values):
            terms[index, :coil_share] = values[centre]
            gaps = []
            for offset in range(1, KSIZE):
                upper = values[centre + offset]
                lower = values[centre - offset]
                row = offset * coil_share
                terms[index, row : row + coil_share] = jnp.where(own_lane, upper, upper + lower)
                gaps.append(upper - lower)
            row = KSIZE * coil_share
            for pair in range(2):
                moved = pltpu.roll(gaps[2 * pair + 1], toward_own, 1)
                terms[index, row : row + coil_share] = jnp.where(own_lane, moved, gaps[2 * pair])
                row += coil_share
            moved = pltpu.roll(gaps[4], toward_own, 1)
            rest = coil_share // 2
            terms[index, row : row + rest] = jnp.where(own_lane[:rest], moved[rest:], gaps[4][:rest])

        def own_sum(q, part):
            mine = keep_ref[q, part, pl.ds(own, coil_share)]
            return (mine + got_ref[q, part].astype(jnp.float32)) * factor

        back = jnp.where(half_ref[0] == 0, WIDE - coil_share, coil_share)

        def other_sum(q, part):
            mine = keep_ref[q, part, pl.ds(other, coil_share)]
            theirs = got_ref[KSIZE + (q - 1) // 2, part].astype(jnp.float32)
            theirs = jnp.where(q % 2 == 1, theirs, pltpu.roll(theirs, back, 1))
            return (mine + theirs) * factor

        def one_shift(q, carry):
            real = own_sum(q, 0)
            imag = own_sum(q, 1)
            whole[q, 0] = real
            whole[q, 1] = imag
            ordered = [real, other_sum(q, 0), -imag, -other_sum(q, 1)]
            turned[...] = jnp.concatenate(ordered + ordered, axis=0).T
            ahead = forward(q)
            sums = []
            gaps = []
            for p in range(SPAN):
                row = pl.multiple_of((SPAN - 1 - p) * COILS + own, coil_share)
                behind = turned[pl.ds(row, coil_share), :]
                sums.append(ahead[p] + behind)
                gaps.append(pltpu.roll(ahead[p] - behind, COILS, 1) * swap_sign)
            place(q, sums)
            place(KSIZE - 1 + q, gaps)
            return carry

        for part in range(2):
            whole[0, part] = own_sum(0, part)
        place(0, forward(0))
        lax.fori_loop(1, KSIZE, one_shift, 0)

    build()
    blocks = table_ref.shape[0]
    group_size = 2

    def one(step, carry):
        places = [step * group_size + extra for extra in range(group_size)]
        weights = [
            [
                jnp.broadcast_to(table_ref[place, index : index + 1, :], (8, LANES))
                for index in range(2 * KSIZE - 2)
            ]
            for place in places
        ]
        for first in range(0, PACKED, coil_share):
            made = [[] for _ in places]
            last = min(first + coil_share, PACKED)
            for row in range(first, last, 8):
                cells = [terms[index, row : row + 8] for index in range(2 * KSIZE - 1)]
                for extra in range(group_size):
                    even = cells[0]
                    odd = None
                    for q in range(1, KSIZE):
                        piece = (
                            cells[q] * weights[extra][q - 1]
                            + cells[KSIZE - 1 + q] * weights[extra][KSIZE - 2 + q]
                        )
                        if q % 2 == 0:
                            even = even + piece
                        else:
                            odd = piece if odd is None else odd + piece
                    made[extra].append((even + odd, even - odd))
            for extra, place in enumerate(places):
                for sign in range(2):
                    whole_rows = jnp.concatenate([half[sign] for half in made[extra]], axis=0)
                    out_ref[place + sign * blocks, first:last, :] = whole_rows.astype(jnp.bfloat16)
        return carry

    lax.fori_loop(0, blocks // group_size, one, 0)


def column_rows(half, keep, got):
    blocks = IMG // 2
    return pl.pallas_call(
        transform_kernel,
        in_specs=[pl.BlockSpec(memory_space=pltpu.SMEM)]
        + [pl.BlockSpec(memory_space=pltpu.VMEM)] * 3,
        out_specs=pl.BlockSpec(memory_space=pltpu.VMEM),
        scratch_shapes=[
            pltpu.VMEM((KSIZE, 2, COILS // 2, WIDE), jnp.float32),
            pltpu.VMEM((WIDE, LANES), jnp.float32),
            pltpu.VMEM((2 * KSIZE - 1, PACKED, LANES), jnp.float32),
        ],
        out_shape=jax.ShapeDtypeStruct((blocks, PACKED, LANES), jnp.bfloat16),
        compiler_params=pltpu.CompilerParams(vmem_limit_bytes=16 * 2**20),
        name="column_rows",
    )(half, keep, got, jnp.asarray(transform_table()))


def phase_table():
    table = np.zeros((16, IMG), np.float32)
    for p in range(1, KSIZE):
        angle = 2.0 * math.pi * ((p * np.arange(IMG)) % IMG) / IMG
        table[p - 1] = np.cos(angle)
        table[KSIZE - 2 + p] = np.sin(angle)
    return table


def apply_kernel(half_ref, rows_ref, maps_ref, table_ref, out_ref, result, even_rows, odd_rows, sems):
    coil_share = COILS // 2
    slices = rows_ref.shape[0]
    waves = [
        jnp.broadcast_to(table_ref[index : index + 1, :], (coil_share, IMG))
        for index in range(2 * KSIZE - 2)
    ]
    blank = jnp.zeros((2 * COILS, 2 * IMG), jnp.bfloat16)
    own = pl.multiple_of(half_ref[0] * coil_share, coil_share)
    other = pl.multiple_of(coil_share - half_ref[0] * coil_share, coil_share)
    lane = lax.broadcasted_iota(jnp.int32, (coil_share, LANES), 1)
    own_lane = lane // coil_share % 2 == 0
    group = lane // COILS
    groups = LANES // COILS
    buffers = (even_rows, odd_rows)

    def unpack(index, lhs, local):
        def tile(place):
            return rows_ref[index, place * coil_share : (place + 1) * coil_share, :]

        def spread(packed):
            return packed, pltpu.roll(packed, coil_share, 1)

        first, second = spread(tile(KSIZE))
        third, fourth = spread(tile(KSIZE + 1))
        tail = spread(rows_ref[index, (KSIZE + 2) * coil_share :, :])
        crossed = [first, second, third, fourth, jnp.concatenate(tail, axis=0)]
        merged = [tile(place) for place in range(KSIZE)]
        stacked = jnp.concatenate(merged[1:] + [jnp.zeros((3 * coil_share, LANES), BF)], axis=0).T
        strips = []
        for target in range(groups):
            strip = stacked[target * COILS : target * COILS + coil_share]
            strips.append(-strip if target % 2 else strip)
        lhs[local, :coil_share] = merged[0]
        for p in range(1, KSIZE):
            mirror = None
            for target in range(groups):
                shift = (target * COILS - (p - 1) * coil_share) % LANES
                moved = pltpu.roll(strips[target], shift, 1) if shift else strips[target]
                mirror = moved if mirror is None else jnp.where(group == target, moved, mirror)
            row = p * coil_share
            lhs[local, row : row + coil_share] = jnp.where(
                own_lane, merged[p] + mirror, merged[p]
            )
            row = (p + KSIZE - 1) * coil_share
            lhs[local, row : row + coil_share] = jnp.where(
                own_lane, merged[p] - mirror, crossed[p - 1]
            )

    def one(index, y, lhs, local):
        real, imag = [
            jnp.concatenate(
                [maps_ref[y, index, part, pl.ds(first, coil_share)] for first in (own, other)],
                axis=0,
            )
            for part in range(2)
        ]
        filled = jnp.concatenate(
            [
                jnp.concatenate([real, imag], axis=1),
                jnp.concatenate([-imag, real], axis=1),
            ],
            axis=0,
        )
        halves = [filled, blank] if y == 0 else [blank, filled]
        mixed = jnp.dot(
            lhs[local], jnp.concatenate(halves, axis=0), preferred_element_type=jnp.float32
        )

        def piece(place, part):
            return mixed[
                place * coil_share : (place + 1) * coil_share, part * IMG : (part + 1) * IMG
            ]

        out_real = piece(0, 0)
        out_imag = piece(0, 1)
        for p in range(1, KSIZE):
            cosine = waves[p - 1]
            sine = waves[KSIZE - 2 + p]
            out_real = out_real + (piece(p, 0) * cosine - piece(KSIZE - 1 + p, 1) * sine)
            out_imag = out_imag + (piece(p, 1) * cosine + piece(KSIZE - 1 + p, 0) * sine)
        result[y, index, 0] = out_real.astype(jnp.bfloat16)
        result[y, index, 1] = out_imag.astype(jnp.bfloat16)

    def write(step):
        span = pl.ds(step * 2 * SBLOCK, 2 * SBLOCK)
        return pltpu.make_async_copy(result.at[:, span], out_ref.at[:, span], sems.at[step])

    def block(step, carry):
        first = step * 2 * SBLOCK
        for current, following in ((0, 1), (1, 0)):
            for local in range(SBLOCK):
                index = first + current * SBLOCK + local
                ahead = jnp.minimum(index + SBLOCK, slices - 1)
                unpack(ahead, buffers[following], local)
                for y in range(2):
                    one(index, y, buffers[current], local)
        write(step).start()
        return carry

    steps = slices // (2 * SBLOCK)
    for local in range(SBLOCK):
        unpack(local, buffers[0], local)
    lax.fori_loop(0, steps, block, 0)
    for step in range(steps):
        write(step).wait()


def apply_rows(half, rows, maps):
    slices = rows.shape[0]
    width = maps.shape[0]
    shape = (width, slices, 2, COILS // 2, IMG)
    return pl.pallas_call(
        apply_kernel,
        in_specs=[pl.BlockSpec(memory_space=pltpu.SMEM)]
        + [pl.BlockSpec(memory_space=pltpu.VMEM)] * 3,
        out_specs=pl.BlockSpec(memory_space=pltpu.HBM),
        out_shape=jax.ShapeDtypeStruct(shape, jnp.bfloat16),
        scratch_shapes=[
            pltpu.VMEM(shape, jnp.bfloat16),
            pltpu.VMEM((SBLOCK, SPAN * COILS // 2, LANES), jnp.bfloat16),
            pltpu.VMEM((SBLOCK, SPAN * COILS // 2, LANES), jnp.bfloat16),
            pltpu.SemaphoreType.DMA((slices // (2 * SBLOCK),)),
        ],
        compiler_params=pltpu.CompilerParams(vmem_limit_bytes=16 * 2**20),
        name="apply_rows",
    )(half, rows, maps, jnp.asarray(phase_table()))


def shards(basis, picks, coil_maps):
    half = lax.axis_index("col").astype(jnp.int32).reshape(1)
    keep, send = partial_kernels(half, basis[0], picks)
    got = lax.ppermute(send, "col", [(0, 1), (1, 0)])
    rows = column_rows(half, keep, got)
    rows = lax.all_to_all(rows, "slc", split_axis=0, concat_axis=0, tiled=True)
    return apply_rows(half, rows, coil_maps)


def solution(mesh):
    placed = (P("slc", None, None, "col"), P("slc", "col"), P("slc", None, None, None, None))
    return jax.shard_map(
        shards,
        mesh=mesh,
        in_specs=placed,
        out_specs=P("slc", None, None, "col", None),
        check_vma=False,
    )
```

```python
import math

import jax
import jax.numpy as jnp
import numpy as np
from jax import lax
from jax.experimental import pallas as pl
from jax.experimental.pallas import tpu as pltpu
from jax.sharding import PartitionSpec as P

COILS = 32
KSIZE = 6
RANK = 608
IMG = 128
SPAN = 2 * KSIZE - 1
LANES = 128
AROWS = KSIZE * COILS
WIDE = 384
SBLOCK = 16
PACKED = 136
DEPTH = 2
BF = jnp.bfloat16


def gram_kernel(
    half_ref, picks_ref, basis_ref, keep_ref, send_ref,
    chosen, buffer, onehot, picked, rows, left, right, pairs, sems, pick_sem,
):
    windows = basis_ref.shape[1]
    width = basis_ref.shape[2]
    used = picks_ref.shape[1]
    coil_share = COILS // 2
    own = pl.multiple_of(half_ref[0] * coil_share, coil_share)
    other = pl.multiple_of(coil_share - half_ref[0] * coil_share, coil_share)
    cuts = [(0, 512), (512, width - 512)]
    fetch = pltpu.make_async_copy(picks_ref, chosen, pick_sem.at[0])
    fetch.start()
    copies = [
        pltpu.make_async_copy(
            basis_ref.at[part, :, pl.ds(first, size)],
            buffer.at[part, :, pl.ds(first, size)],
            sems.at[part, index],
        )
        for part in range(2)
        for index, (first, size) in enumerate(cuts)
    ]
    for copy in copies[:DEPTH]:
        copy.start()

    right[:, AROWS:, :] = jnp.zeros((2, right.shape[1] - AROWS, right.shape[2]), jnp.bfloat16)
    for slot in range(2):
        picked[slot, used:] = jnp.zeros((WIDE - used, picked.shape[2]), jnp.float32)
    fetch.wait()
    wanted = jnp.concatenate([chosen[...], jnp.full((1, WIDE - used), -1, jnp.int32)], axis=1)
    wanted = jnp.broadcast_to(wanted, (LANES, WIDE)).T[:used]
    lane = lax.broadcasted_iota(jnp.int32, (used, LANES), 1)
    for first in range(0, windows, LANES):
        size = min(LANES, windows - first)
        match = jnp.where(wanted == lane + first, 1.0, 0.0).astype(jnp.bfloat16)
        onehot[:, first : first + size] = match[:, :size]

    def spread(position):
        part, index = divmod(position, len(cuts))
        first, size = cuts[index]
        for tile in range(WIDE // LANES):
            rows[part, tile, first : first + size] = picked[
                position % 2, tile * LANES : (tile + 1) * LANES, :size
            ].T
        if index + 1 < len(cuts):
            return
        for a in range(KSIZE):
            for b in range(KSIZE):
                for tile in range(WIDE // LANES):
                    block = rows[
                        part, tile, pl.ds(a * KSIZE + b, COILS, stride=KSIZE * KSIZE), :
                    ].astype(jnp.bfloat16)
                    row = slice(a * COILS, (a + 1) * COILS)
                    spot = slice(b * WIDE + tile * LANES, b * WIDE + (tile + 1) * LANES)
                    left[part, row, spot] = block
                    right[part, row, spot] = block

    for position, copy in enumerate(copies):
        part, index = divmod(position, len(cuts))
        first, size = cuts[index]
        copy.wait()
        if position + DEPTH < len(copies):
            copies[position + DEPTH].start()
        picked[position % 2, :used, :size] = jnp.dot(
            onehot[...],
            buffer[part, :, first : first + size],
            preferred_element_type=jnp.float32,
        )
        if position:
            spread(position - 1)
    spread(len(copies) - 1)

    def against(q, part):
        depth = (KSIZE - q) * WIDE
        lhs = left[:, :, :depth].reshape(2 * AROWS, depth)
        return lax.dot_general(
            lhs,
            right[part, :, q * WIDE :],
            (((1,), (1,)), ((), ())),
            preferred_element_type=jnp.float32,
        )

    pad = jnp.zeros((COILS, WIDE - right.shape[1]), jnp.float32)

    def shift_sums(q):
        for part in range(2):
            total = None
            for a in range(KSIZE):
                block = pairs[q % 2, part, a * COILS : (a + 1) * COILS]
                block = jnp.concatenate([block, pad], axis=1)
                shift = (KSIZE - 1 - a) * COILS
                moved = pltpu.roll(block, shift, 1) if shift else block
                total = moved if total is None else total + moved
            keep_ref[q, part] = total
            send_ref[q, part] = keep_ref[q, part, pl.ds(other, coil_share)].astype(jnp.bfloat16)

    for q in range(KSIZE):
        with_real = against(q, 0)
        with_imag = against(q, 1)
        pairs[q % 2, 0] = with_real[:AROWS] + with_imag[AROWS:]
        pairs[q % 2, 1] = with_real[AROWS:] - with_imag[:AROWS]
        if q:
            shift_sums(q - 1)
    shift_sums(KSIZE - 1)
    lane = lax.broadcasted_iota(jnp.int32, (coil_share, WIDE), 1)
    theirs = lane // coil_share % 2 == 1 - half_ref[0]
    toward = jnp.where(half_ref[0] == 0, WIDE - coil_share, coil_share)
    for q in range(1, KSIZE, 2):
        for part in range(2):
            mixed = keep_ref[q, part, pl.ds(own, coil_share)]
            if q + 1 < KSIZE:
                extra = pltpu.roll(keep_ref[q + 1, part, pl.ds(own, coil_share)], toward, 1)
                mixed = jnp.where(theirs, mixed, extra)
            send_ref[KSIZE + q // 2, part] = mixed.astype(jnp.bfloat16)


def partial_kernels(half, basis, picks):
    turned = pltpu.with_memory_space_constraint(jnp.transpose(basis, (0, 2, 1)), pltpu.HBM)
    picks = pltpu.with_memory_space_constraint(picks, pltpu.HBM)
    parts, windows, rows = turned.shape
    used = picks.shape[1]
    return pl.pallas_call(
        gram_kernel,
        in_specs=[pl.BlockSpec(memory_space=pltpu.SMEM)]
        + [pl.BlockSpec(memory_space=pltpu.HBM)] * 2,
        out_specs=[pl.BlockSpec(memory_space=pltpu.VMEM)] * 2,
        out_shape=[
            jax.ShapeDtypeStruct((KSIZE, 2, COILS, WIDE), jnp.float32),
            jax.ShapeDtypeStruct((KSIZE + KSIZE // 2, 2, COILS // 2, WIDE), jnp.bfloat16),
        ],
        scratch_shapes=[
            pltpu.VMEM((1, used), jnp.int32),
            pltpu.VMEM((parts, windows, rows), jnp.bfloat16),
            pltpu.VMEM((used, windows), jnp.bfloat16),
            pltpu.VMEM((2, WIDE, 640), jnp.float32),
            pltpu.VMEM((parts, WIDE // LANES, rows, LANES), jnp.float32),
            pltpu.VMEM((2, AROWS, KSIZE * WIDE), jnp.bfloat16),
            pltpu.VMEM((2, 256, KSIZE * WIDE), jnp.bfloat16),
            pltpu.VMEM((2, 2, AROWS, 256), jnp.float32),
            pltpu.SemaphoreType.DMA((parts, 3)),
            pltpu.SemaphoreType.DMA((1,)),
        ],
        compiler_params=pltpu.CompilerParams(vmem_limit_bytes=28 * 2**20),
        name="partial_kernels",
    )(half, picks, turned)


def transform_table():
    half = IMG // 4
    table = np.zeros((half, 16, LANES), np.float32)
    for first in range(half):
        for q in range(1, KSIZE):
            lanes_y = np.repeat(2 * first + np.arange(2), LANES // 2)
            angle = 2.0 * math.pi * ((q * lanes_y) % IMG) / IMG
            table[first, q - 1] = np.cos(angle)
            table[first, KSIZE - 2 + q] = np.sin(angle)
    return table


def transform_kernel(half_ref, keep_ref, got_ref, table_ref, out_ref, whole, turned, terms):
    coil_share = COILS // 2

    def build():
        factor = 1.0 / (2.0 * RANK * KSIZE * KSIZE)
        own = pl.multiple_of(half_ref[0] * coil_share, coil_share)
        other = pl.multiple_of(coil_share - half_ref[0] * coil_share, coil_share)
        lane = lax.broadcasted_iota(jnp.int32, (coil_share, LANES), 1)
        group = lane // COILS
        even_slot = group % 2 == 0
        low_half = lane < LANES // 2
        swap_sign = jnp.where(even_slot, -1.0, 1.0)
        centre = KSIZE - 1

        own_lane = lane // coil_share % 2 == 0
        upper_half = half_ref[0] == 1

        def own_first(value):
            down = pltpu.roll(value, LANES - coil_share, 1)
            up = pltpu.roll(value, coil_share, 1)
            return jnp.where(upper_half, jnp.where(own_lane, down, up), value)

        def forward(q):
            found = []
            for tile in range(WIDE // LANES):
                lanes = slice(tile * LANES, (tile + 1) * LANES)
                real = own_first(whole[q, 0, :, lanes])
                imag = own_first(whole[q, 1, :, lanes])
                first = jnp.where(even_slot, real, pltpu.roll(imag, COILS, 1))
                second = jnp.where(even_slot, pltpu.roll(real, LANES - COILS, 1), imag)
                first_turned = pltpu.roll(first, LANES // 2, 1)
                second_turned = pltpu.roll(second, LANES // 2, 1)
                found += [
                    jnp.where(low_half, first, first_turned),
                    jnp.where(low_half, second, second_turned),
                    jnp.where(low_half, first_turned, first),
                    jnp.where(low_half, second_turned, second),
                ]
            return found[:SPAN]

        toward_own = LANES - coil_share

        def place(index, values):
            terms[index, :coil_share] = values[centre]
            gaps = []
            for offset in range(1, KSIZE):
                upper = values[centre + offset]
                lower = values[centre - offset]
                row = offset * coil_share
                terms[index, row : row + coil_share] = jnp.where(own_lane, upper, upper + lower)
                gaps.append(upper - lower)
            row = KSIZE * coil_share
            for pair in range(2):
                moved = pltpu.roll(gaps[2 * pair + 1], toward_own, 1)
                terms[index, row : row + coil_share] = jnp.where(own_lane, moved, gaps[2 * pair])
                row += coil_share
            moved = pltpu.roll(gaps[4], toward_own, 1)
            rest = coil_share // 2
            terms[index, row : row + rest] = jnp.where(own_lane[:rest], moved[rest:], gaps[4][:rest])

        def own_sum(q, part):
            mine = keep_ref[q, part, pl.ds(own, coil_share)]
            return (mine + got_ref[q, part].astype(jnp.float32)) * factor

        back = jnp.where(half_ref[0] == 0, WIDE - coil_share, coil_share)

        def other_sum(q, part):
            mine = keep_ref[q, part, pl.ds(other, coil_share)]
            theirs = got_ref[KSIZE + (q - 1) // 2, part].astype(jnp.float32)
            theirs = jnp.where(q % 2 == 1, theirs, pltpu.roll(theirs, back, 1))
            return (mine + theirs) * factor

        def one_shift(q, carry):
            real = own_sum(q, 0)
            imag = own_sum(q, 1)
            whole[q, 0] = real
            whole[q, 1] = imag
            ordered = [real, other_sum(q, 0), -imag, -other_sum(q, 1)]
            turned[...] = jnp.concatenate(ordered + ordered, axis=0).T
            ahead = forward(q)
            sums = []
            gaps = []
            for p in range(SPAN):
                row = pl.multiple_of((SPAN - 1 - p) * COILS + own, coil_share)
                behind = turned[pl.ds(row, coil_share), :]
                sums.append(ahead[p] + behind)
                gaps.append(pltpu.roll(ahead[p] - behind, COILS, 1) * swap_sign)
            place(q, sums)
            place(KSIZE - 1 + q, gaps)
            return carry

        for part in range(2):
            whole[0, part] = own_sum(0, part)
        place(0, forward(0))
        lax.fori_loop(1, KSIZE, one_shift, 0)

    build()
    blocks = table_ref.shape[0]
    group_size = 2

    def one(step, carry):
        places = [step * group_size + extra for extra in range(group_size)]
        weights = [
            [
                jnp.broadcast_to(table_ref[place, index : index + 1, :], (8, LANES))
                for index in range(2 * KSIZE - 2)
            ]
            for place in places
        ]
        for first in range(0, PACKED, coil_share):
            made = [[] for _ in places]
            last = min(first + coil_share, PACKED)
            for row in range(first, last, 8):
                cells = [terms[index, row : row + 8] for index in range(2 * KSIZE - 1)]
                for extra in range(group_size):
                    even = cells[0]
                    odd = None
                    for q in range(1, KSIZE):
                        piece = (
                            cells[q] * weights[extra][q - 1]
                            + cells[KSIZE - 1 + q] * weights[extra][KSIZE - 2 + q]
                        )
                        if q % 2 == 0:
                            even = even + piece
                        else:
                            odd = piece if odd is None else odd + piece
                    made[extra].append((even + odd, even - odd))
            for extra, place in enumerate(places):
                for sign in range(2):
                    whole_rows = jnp.concatenate([half[sign] for half in made[extra]], axis=0)
                    out_ref[place + sign * blocks, first:last, :] = whole_rows.astype(jnp.bfloat16)
        return carry

    lax.fori_loop(0, blocks // group_size, one, 0)


def column_rows(half, keep, got):
    blocks = IMG // 2
    return pl.pallas_call(
        transform_kernel,
        in_specs=[pl.BlockSpec(memory_space=pltpu.SMEM)]
        + [pl.BlockSpec(memory_space=pltpu.VMEM)] * 3,
        out_specs=pl.BlockSpec(memory_space=pltpu.VMEM),
        scratch_shapes=[
            pltpu.VMEM((KSIZE, 2, COILS // 2, WIDE), jnp.float32),
            pltpu.VMEM((WIDE, LANES), jnp.float32),
            pltpu.VMEM((2 * KSIZE - 1, PACKED, LANES), jnp.float32),
        ],
        out_shape=jax.ShapeDtypeStruct((blocks, PACKED, LANES), jnp.bfloat16),
        compiler_params=pltpu.CompilerParams(vmem_limit_bytes=16 * 2**20),
        name="column_rows",
    )(half, keep, got, jnp.asarray(transform_table()))


def phase_table():
    table = np.zeros((16, IMG), np.float32)
    for p in range(1, KSIZE):
        angle = 2.0 * math.pi * ((p * np.arange(IMG)) % IMG) / IMG
        table[p - 1] = np.cos(angle)
        table[KSIZE - 2 + p] = np.sin(angle)
    return table


def apply_kernel(half_ref, rows_ref, maps_ref, table_ref, out_ref, result, even_rows, odd_rows, sems):
    coil_share = COILS // 2
    slices = rows_ref.shape[0]
    waves = [
        jnp.broadcast_to(table_ref[index : index + 1, :], (coil_share, IMG))
        for index in range(2 * KSIZE - 2)
    ]
    blank = jnp.zeros((2 * COILS, 2 * IMG), jnp.bfloat16)
    own = pl.multiple_of(half_ref[0] * coil_share, coil_share)
    other = pl.multiple_of(coil_share - half_ref[0] * coil_share, coil_share)
    lane = lax.broadcasted_iota(jnp.int32, (coil_share, LANES), 1)
    own_lane = lane // coil_share % 2 == 0
    group = lane // COILS
    groups = LANES // COILS
    buffers = (even_rows, odd_rows)

    def unpack(index, lhs, local):
        def tile(place):
            return rows_ref[index, place * coil_share : (place + 1) * coil_share, :]

        def spread(packed):
            return packed, pltpu.roll(packed, coil_share, 1)

        first, second = spread(tile(KSIZE))
        third, fourth = spread(tile(KSIZE + 1))
        tail = spread(rows_ref[index, (KSIZE + 2) * coil_share :, :])
        crossed = [first, second, third, fourth, jnp.concatenate(tail, axis=0)]
        merged = [tile(place) for place in range(KSIZE)]
        stacked = jnp.concatenate(merged[1:] + [jnp.zeros((3 * coil_share, LANES), BF)], axis=0).T
        strips = []
        for target in range(groups):
            strip = stacked[target * COILS : target * COILS + coil_share]
            strips.append(-strip if target % 2 else strip)
        lhs[local, :coil_share] = merged[0]
        for p in range(1, KSIZE):
            mirror = None
            for target in range(groups):
                shift = (target * COILS - (p - 1) * coil_share) % LANES
                moved = pltpu.roll(strips[target], shift, 1) if shift else strips[target]
                mirror = moved if mirror is None else jnp.where(group == target, moved, mirror)
            row = p * coil_share
            lhs[local, row : row + coil_share] = jnp.where(
                own_lane, merged[p] + mirror, merged[p]
            )
            row = (p + KSIZE - 1) * coil_share
            lhs[local, row : row + coil_share] = jnp.where(
                own_lane, merged[p] - mirror, crossed[p - 1]
            )

    def one(index, y, lhs, local):
        real, imag = [
            jnp.concatenate(
                [maps_ref[y, index, part, pl.ds(first, coil_share)] for first in (own, other)],
                axis=0,
            )
            for part in range(2)
        ]
        filled = jnp.concatenate(
            [
                jnp.concatenate([real, imag], axis=1),
                jnp.concatenate([-imag, real], axis=1),
            ],
            axis=0,
        )
        halves = [filled, blank] if y == 0 else [blank, filled]
        mixed = jnp.dot(
            lhs[local], jnp.concatenate(halves, axis=0), preferred_element_type=jnp.float32
        )

        def piece(place, part):
            return mixed[
                place * coil_share : (place + 1) * coil_share, part * IMG : (part + 1) * IMG
            ]

        out_real = piece(0, 0)
        out_imag = piece(0, 1)
        for p in range(1, KSIZE):
            cosine = waves[p - 1]
            sine = waves[KSIZE - 2 + p]
            out_real = out_real + (piece(p, 0) * cosine - piece(KSIZE - 1 + p, 1) * sine)
            out_imag = out_imag + (piece(p, 1) * cosine + piece(KSIZE - 1 + p, 0) * sine)
        result[y, index, 0] = out_real.astype(jnp.bfloat16)
        result[y, index, 1] = out_imag.astype(jnp.bfloat16)

    def write(step):
        span = pl.ds(step * 2 * SBLOCK, 2 * SBLOCK)
        return pltpu.make_async_copy(result.at[:, span], out_ref.at[:, span], sems.at[step])

    def block(step, carry):
        first = step * 2 * SBLOCK
        for current, following in ((0, 1), (1, 0)):
            for local in range(SBLOCK):
                index = first + current * SBLOCK + local
                ahead = jnp.minimum(index + SBLOCK, slices - 1)
                unpack(ahead, buffers[following], local)
                for y in range(2):
                    one(index, y, buffers[current], local)
        write(step).start()
        return carry

    steps = slices // (2 * SBLOCK)
    for local in range(SBLOCK):
        unpack(local, buffers[0], local)
    lax.fori_loop(0, steps, block, 0)
    for step in range(steps):
        write(step).wait()


def apply_rows(half, rows, maps):
    slices = rows.shape[0]
    width = maps.shape[0]
    shape = (width, slices, 2, COILS // 2, IMG)
    return pl.pallas_call(
        apply_kernel,
        in_specs=[pl.BlockSpec(memory_space=pltpu.SMEM)]
        + [pl.BlockSpec(memory_space=pltpu.VMEM)] * 3,
        out_specs=pl.BlockSpec(memory_space=pltpu.HBM),
        out_shape=jax.ShapeDtypeStruct(shape, jnp.bfloat16),
        scratch_shapes=[
            pltpu.VMEM(shape, jnp.bfloat16),
            pltpu.VMEM((SBLOCK, SPAN * COILS // 2, LANES), jnp.bfloat16),
            pltpu.VMEM((SBLOCK, SPAN * COILS // 2, LANES), jnp.bfloat16),
            pltpu.SemaphoreType.DMA((slices // (2 * SBLOCK),)),
        ],
        compiler_params=pltpu.CompilerParams(vmem_limit_bytes=16 * 2**20),
        name="apply_rows",
    )(half, rows, maps, jnp.asarray(phase_table()))


def shards(basis, picks, coil_maps):
    half = lax.axis_index("col").astype(jnp.int32).reshape(1)
    keep, send = partial_kernels(half, basis[0], picks)
    got = lax.ppermute(send, "col", [(0, 1), (1, 0)])
    rows = column_rows(half, keep, got)
    rows = lax.all_to_all(rows, "slc", split_axis=0, concat_axis=0, tiled=True)
    return apply_rows(half, rows, coil_maps)


def solution(mesh):
    placed = (P("slc", None, None, "col"), P("slc", "col"), P("slc", None, None, None, None))
    return jax.shard_map(
        shards,
        mesh=mesh,
        in_specs=placed,
        out_specs=P("slc", None, None, "col", None),
        check_vma=False,
    )
```

```python
import math

import jax
import jax.numpy as jnp
import numpy as np
from jax import lax
from jax.experimental import pallas as pl
from jax.experimental.pallas import tpu as pltpu
from jax.sharding import PartitionSpec as P

COILS = 32
KSIZE = 6
RANK = 608
IMG = 128
SPAN = 2 * KSIZE - 1
LANES = 128
AROWS = KSIZE * COILS
WIDE = 384
SBLOCK = 16
PACKED = 136
DEPTH = 2
BF = jnp.bfloat16


def gram_kernel(
    half_ref, picks_ref, basis_ref, keep_ref, send_ref,
    chosen, buffer, onehot, picked, rows, left, right, pairs, sems, pick_sem,
):
    windows = basis_ref.shape[1]
    width = basis_ref.shape[2]
    used = picks_ref.shape[1]
    coil_share = COILS // 2
    own = pl.multiple_of(half_ref[0] * coil_share, coil_share)
    other = pl.multiple_of(coil_share - half_ref[0] * coil_share, coil_share)
    cuts = [(0, 512), (512, width - 512)]
    fetch = pltpu.make_async_copy(picks_ref, chosen, pick_sem.at[0])
    fetch.start()
    copies = [
        pltpu.make_async_copy(
            basis_ref.at[part, :, pl.ds(first, size)],
            buffer.at[part, :, pl.ds(first, size)],
            sems.at[part, index],
        )
        for part in range(2)
        for index, (first, size) in enumerate(cuts)
    ]
    for copy in copies[:DEPTH]:
        copy.start()

    right[:, AROWS:, :] = jnp.zeros((2, right.shape[1] - AROWS, right.shape[2]), jnp.bfloat16)
    for slot in range(2):
        picked[slot, used:] = jnp.zeros((WIDE - used, picked.shape[2]), jnp.float32)
    fetch.wait()
    wanted = jnp.concatenate([chosen[...], jnp.full((1, WIDE - used), -1, jnp.int32)], axis=1)
    wanted = jnp.broadcast_to(wanted, (LANES, WIDE)).T[:used]
    lane = lax.broadcasted_iota(jnp.int32, (used, LANES), 1)
    for first in range(0, windows, LANES):
        size = min(LANES, windows - first)
        match = jnp.where(wanted == lane + first, 1.0, 0.0).astype(jnp.bfloat16)
        onehot[:, first : first + size] = match[:, :size]

    def spread(position):
        part, index = divmod(position, len(cuts))
        first, size = cuts[index]
        for tile in range(WIDE // LANES):
            rows[part, tile, first : first + size] = picked[
                position % 2, tile * LANES : (tile + 1) * LANES, :size
            ].T
        if index + 1 < len(cuts):
            return
        for a in range(KSIZE):
            for b in range(KSIZE):
                for tile in range(WIDE // LANES):
                    block = rows[
                        part, tile, pl.ds(a * KSIZE + b, COILS, stride=KSIZE * KSIZE), :
                    ].astype(jnp.bfloat16)
                    row = slice(a * COILS, (a + 1) * COILS)
                    spot = slice(b * WIDE + tile * LANES, b * WIDE + (tile + 1) * LANES)
                    left[part, row, spot] = block
                    right[part, row, spot] = block

    for position, copy in enumerate(copies):
        part, index = divmod(position, len(cuts))
        first, size = cuts[index]
        copy.wait()
        if position + DEPTH < len(copies):
            copies[position + DEPTH].start()
        picked[position % 2, :used, :size] = jnp.dot(
            onehot[...],
            buffer[part, :, first : first + size],
            preferred_element_type=jnp.float32,
        )
        if position:
            spread(position - 1)
    spread(len(copies) - 1)

    def against(q, part):
        depth = (KSIZE - q) * WIDE
        lhs = left[:, :, :depth].reshape(2 * AROWS, depth)
        return lax.dot_general(
            lhs,
            right[part, :, q * WIDE :],
            (((1,), (1,)), ((), ())),
            preferred_element_type=jnp.float32,
        )

    pad = jnp.zeros((COILS, WIDE - right.shape[1]), jnp.float32)

    def shift_sums(q):
        for part in range(2):
            total = None
            for a in range(KSIZE):
                block = pairs[q % 2, part, a * COILS : (a + 1) * COILS]
                block = jnp.concatenate([block, pad], axis=1)
                shift = (KSIZE - 1 - a) * COILS
                moved = pltpu.roll(block, shift, 1) if shift else block
                total = moved if total is None else total + moved
            keep_ref[q, part] = total
            send_ref[q, part] = keep_ref[q, part, pl.ds(other, coil_share)].astype(jnp.bfloat16)

    for q in range(KSIZE):
        with_real = against(q, 0)
        with_imag = against(q, 1)
        pairs[q % 2, 0] = with_real[:AROWS] + with_imag[AROWS:]
        pairs[q % 2, 1] = with_real[AROWS:] - with_imag[:AROWS]
        if q:
            shift_sums(q - 1)
    shift_sums(KSIZE - 1)
    lane = lax.broadcasted_iota(jnp.int32, (coil_share, WIDE), 1)
    theirs = lane // coil_share % 2 == 1 - half_ref[0]
    toward = jnp.where(half_ref[0] == 0, WIDE - coil_share, coil_share)
    for q in range(1, KSIZE, 2):
        for part in range(2):
            mixed = keep_ref[q, part, pl.ds(own, coil_share)]
            if q + 1 < KSIZE:
                extra = pltpu.roll(keep_ref[q + 1, part, pl.ds(own, coil_share)], toward, 1)
                mixed = jnp.where(theirs, mixed, extra)
            send_ref[KSIZE + q // 2, part] = mixed.astype(jnp.bfloat16)


def partial_kernels(half, basis, picks):
    turned = pltpu.with_memory_space_constraint(jnp.transpose(basis, (0, 2, 1)), pltpu.HBM)
    picks = pltpu.with_memory_space_constraint(picks, pltpu.HBM)
    parts, windows, rows = turned.shape
    used = picks.shape[1]
    return pl.pallas_call(
        gram_kernel,
        in_specs=[pl.BlockSpec(memory_space=pltpu.SMEM)]
        + [pl.BlockSpec(memory_space=pltpu.HBM)] * 2,
        out_specs=[pl.BlockSpec(memory_space=pltpu.VMEM)] * 2,
        out_shape=[
            jax.ShapeDtypeStruct((KSIZE, 2, COILS, WIDE), jnp.float32),
            jax.ShapeDtypeStruct((KSIZE + KSIZE // 2, 2, COILS // 2, WIDE), jnp.bfloat16),
        ],
        scratch_shapes=[
            pltpu.VMEM((1, used), jnp.int32),
            pltpu.VMEM((parts, windows, rows), jnp.bfloat16),
            pltpu.VMEM((used, windows), jnp.bfloat16),
            pltpu.VMEM((2, WIDE, 640), jnp.float32),
            pltpu.VMEM((parts, WIDE // LANES, rows, LANES), jnp.float32),
            pltpu.VMEM((2, AROWS, KSIZE * WIDE), jnp.bfloat16),
            pltpu.VMEM((2, 256, KSIZE * WIDE), jnp.bfloat16),
            pltpu.VMEM((2, 2, AROWS, 256), jnp.float32),
            pltpu.SemaphoreType.DMA((parts, 3)),
            pltpu.SemaphoreType.DMA((1,)),
        ],
        compiler_params=pltpu.CompilerParams(vmem_limit_bytes=28 * 2**20),
        name="partial_kernels",
    )(half, picks, turned)


def transform_table():
    half = IMG // 4
    table = np.zeros((half, 16, LANES), np.float32)
    for first in range(half):
        for q in range(1, KSIZE):
            lanes_y = np.repeat(2 * first + np.arange(2), LANES // 2)
            angle = 2.0 * math.pi * ((q * lanes_y) % IMG) / IMG
            table[first, q - 1] = np.cos(angle)
            table[first, KSIZE - 2 + q] = np.sin(angle)
    return table


def transform_kernel(half_ref, keep_ref, got_ref, table_ref, out_ref, whole, turned, terms):
    coil_share = COILS // 2

    def build():
        factor = 1.0 / (2.0 * RANK * KSIZE * KSIZE)
        own = pl.multiple_of(half_ref[0] * coil_share, coil_share)
        other = pl.multiple_of(coil_share - half_ref[0] * coil_share, coil_share)
        lane = lax.broadcasted_iota(jnp.int32, (coil_share, LANES), 1)
        group = lane // COILS
        even_slot = group % 2 == 0
        low_half = lane < LANES // 2
        swap_sign = jnp.where(even_slot, -1.0, 1.0)
        centre = KSIZE - 1

        own_lane = lane // coil_share % 2 == 0
        upper_half = half_ref[0] == 1

        def own_first(value):
            down = pltpu.roll(value, LANES - coil_share, 1)
            up = pltpu.roll(value, coil_share, 1)
            return jnp.where(upper_half, jnp.where(own_lane, down, up), value)

        def forward(q):
            found = []
            for tile in range(WIDE // LANES):
                lanes = slice(tile * LANES, (tile + 1) * LANES)
                real = own_first(whole[q, 0, :, lanes])
                imag = own_first(whole[q, 1, :, lanes])
                first = jnp.where(even_slot, real, pltpu.roll(imag, COILS, 1))
                second = jnp.where(even_slot, pltpu.roll(real, LANES - COILS, 1), imag)
                first_turned = pltpu.roll(first, LANES // 2, 1)
                second_turned = pltpu.roll(second, LANES // 2, 1)
                found += [
                    jnp.where(low_half, first, first_turned),
                    jnp.where(low_half, second, second_turned),
                    jnp.where(low_half, first_turned, first),
                    jnp.where(low_half, second_turned, second),
                ]
            return found[:SPAN]

        toward_own = LANES - coil_share

        def place(index, values):
            terms[index, :coil_share] = values[centre]
            gaps = []
            for offset in range(1, KSIZE):
                upper = values[centre + offset]
                lower = values[centre - offset]
                row = offset * coil_share
                terms[index, row : row + coil_share] = jnp.where(own_lane, upper, upper + lower)
                gaps.append(upper - lower)
            row = KSIZE * coil_share
            for pair in range(2):
                moved = pltpu.roll(gaps[2 * pair + 1], toward_own, 1)
                terms[index, row : row + coil_share] = jnp.where(own_lane, moved, gaps[2 * pair])
                row += coil_share
            moved = pltpu.roll(gaps[4], toward_own, 1)
            rest = coil_share // 2
            terms[index, row : row + rest] = jnp.where(own_lane[:rest], moved[rest:], gaps[4][:rest])

        def own_sum(q, part):
            mine = keep_ref[q, part, pl.ds(own, coil_share)]
            return (mine + got_ref[q, part].astype(jnp.float32)) * factor

        back = jnp.where(half_ref[0] == 0, WIDE - coil_share, coil_share)

        def other_sum(q, part):
            mine = keep_ref[q, part, pl.ds(other, coil_share)]
            theirs = got_ref[KSIZE + (q - 1) // 2, part].astype(jnp.float32)
            theirs = jnp.where(q % 2 == 1, theirs, pltpu.roll(theirs, back, 1))
            return (mine + theirs) * factor

        def one_shift(q, carry):
            real = own_sum(q, 0)
            imag = own_sum(q, 1)
            whole[q, 0] = real
            whole[q, 1] = imag
            ordered = [real, other_sum(q, 0), -imag, -other_sum(q, 1)]
            turned[...] = jnp.concatenate(ordered + ordered, axis=0).T
            ahead = forward(q)
            sums = []
            gaps = []
            for p in range(SPAN):
                row = pl.multiple_of((SPAN - 1 - p) * COILS + own, coil_share)
                behind = turned[pl.ds(row, coil_share), :]
                sums.append(ahead[p] + behind)
                gaps.append(pltpu.roll(ahead[p] - behind, COILS, 1) * swap_sign)
            place(q, sums)
            place(KSIZE - 1 + q, gaps)
            return carry

        for part in range(2):
            whole[0, part] = own_sum(0, part)
        place(0, forward(0))
        lax.fori_loop(1, KSIZE, one_shift, 0)

    build()
    blocks = table_ref.shape[0]
    group_size = 4

    def one(step, carry):
        places = [step * group_size + extra for extra in range(group_size)]
        weights = [
            [
                jnp.broadcast_to(table_ref[place, index : index + 1, :], (8, LANES))
                for index in range(2 * KSIZE - 2)
            ]
            for place in places
        ]
        for first in range(0, PACKED, coil_share):
            made = [[] for _ in places]
            last = min(first + coil_share, PACKED)
            for row in range(first, last, 8):
                cells = [terms[index, row : row + 8] for index in range(2 * KSIZE - 1)]
                for extra in range(group_size):
                    even = cells[0]
                    odd = None
                    for q in range(1, KSIZE):
                        piece = (
                            cells[q] * weights[extra][q - 1]
                            + cells[KSIZE - 1 + q] * weights[extra][KSIZE - 2 + q]
                        )
                        if q % 2 == 0:
                            even = even + piece
                        else:
                            odd = piece if odd is None else odd + piece
                    made[extra].append((even + odd, even - odd))
            for extra, place in enumerate(places):
                for sign in range(2):
                    whole_rows = jnp.concatenate([half[sign] for half in made[extra]], axis=0)
                    out_ref[place + sign * blocks, first:last, :] = whole_rows.astype(jnp.bfloat16)
        return carry

    lax.fori_loop(0, blocks // group_size, one, 0)


def column_rows(half, keep, got):
    blocks = IMG // 2
    return pl.pallas_call(
        transform_kernel,
        in_specs=[pl.BlockSpec(memory_space=pltpu.SMEM)]
        + [pl.BlockSpec(memory_space=pltpu.VMEM)] * 3,
        out_specs=pl.BlockSpec(memory_space=pltpu.VMEM),
        scratch_shapes=[
            pltpu.VMEM((KSIZE, 2, COILS // 2, WIDE), jnp.float32),
            pltpu.VMEM((WIDE, LANES), jnp.float32),
            pltpu.VMEM((2 * KSIZE - 1, PACKED, LANES), jnp.float32),
        ],
        out_shape=jax.ShapeDtypeStruct((blocks, PACKED, LANES), jnp.bfloat16),
        compiler_params=pltpu.CompilerParams(vmem_limit_bytes=16 * 2**20),
        name="column_rows",
    )(half, keep, got, jnp.asarray(transform_table()))


def phase_table():
    table = np.zeros((16, IMG), np.float32)
    for p in range(1, KSIZE):
        angle = 2.0 * math.pi * ((p * np.arange(IMG)) % IMG) / IMG
        table[p - 1] = np.cos(angle)
        table[KSIZE - 2 + p] = np.sin(angle)
    return table


def apply_kernel(half_ref, rows_ref, maps_ref, table_ref, out_ref, result, even_rows, odd_rows, sems):
    coil_share = COILS // 2
    slices = rows_ref.shape[0]
    waves = [
        jnp.broadcast_to(table_ref[index : index + 1, :], (coil_share, IMG))
        for index in range(2 * KSIZE - 2)
    ]
    blank = jnp.zeros((2 * COILS, 2 * IMG), jnp.bfloat16)
    own = pl.multiple_of(half_ref[0] * coil_share, coil_share)
    other = pl.multiple_of(coil_share - half_ref[0] * coil_share, coil_share)
    lane = lax.broadcasted_iota(jnp.int32, (coil_share, LANES), 1)
    own_lane = lane // coil_share % 2 == 0
    group = lane // COILS
    groups = LANES // COILS
    buffers = (even_rows, odd_rows)

    def unpack(index, lhs, local):
        def tile(place):
            return rows_ref[index, place * coil_share : (place + 1) * coil_share, :]

        def spread(packed):
            return packed, pltpu.roll(packed, coil_share, 1)

        first, second = spread(tile(KSIZE))
        third, fourth = spread(tile(KSIZE + 1))
        tail = spread(rows_ref[index, (KSIZE + 2) * coil_share :, :])
        crossed = [first, second, third, fourth, jnp.concatenate(tail, axis=0)]
        merged = [tile(place) for place in range(KSIZE)]
        stacked = jnp.concatenate(merged[1:] + [jnp.zeros((3 * coil_share, LANES), BF)], axis=0).T
        strips = []
        for target in range(groups):
            strip = stacked[target * COILS : target * COILS + coil_share]
            strips.append(-strip if target % 2 else strip)
        lhs[local, :coil_share] = merged[0]
        for p in range(1, KSIZE):
            mirror = None
            for target in range(groups):
                shift = (target * COILS - (p - 1) * coil_share) % LANES
                moved = pltpu.roll(strips[target], shift, 1) if shift else strips[target]
                mirror = moved if mirror is None else jnp.where(group == target, moved, mirror)
            row = p * coil_share
            lhs[local, row : row + coil_share] = jnp.where(
                own_lane, merged[p] + mirror, merged[p]
            )
            row = (p + KSIZE - 1) * coil_share
            lhs[local, row : row + coil_share] = jnp.where(
                own_lane, merged[p] - mirror, crossed[p - 1]
            )

    def one(index, y, lhs, local):
        real, imag = [
            jnp.concatenate(
                [maps_ref[y, index, part, pl.ds(first, coil_share)] for first in (own, other)],
                axis=0,
            )
            for part in range(2)
        ]
        filled = jnp.concatenate(
            [
                jnp.concatenate([real, imag], axis=1),
                jnp.concatenate([-imag, real], axis=1),
            ],
            axis=0,
        )
        halves = [filled, blank] if y == 0 else [blank, filled]
        mixed = jnp.dot(
            lhs[local], jnp.concatenate(halves, axis=0), preferred_element_type=jnp.float32
        )

        def piece(place, part):
            return mixed[
                place * coil_share : (place + 1) * coil_share, part * IMG : (part + 1) * IMG
            ]

        out_real = piece(0, 0)
        out_imag = piece(0, 1)
        for p in range(1, KSIZE):
            cosine = waves[p - 1]
            sine = waves[KSIZE - 2 + p]
            out_real = out_real + (piece(p, 0) * cosine - piece(KSIZE - 1 + p, 1) * sine)
            out_imag = out_imag + (piece(p, 1) * cosine + piece(KSIZE - 1 + p, 0) * sine)
        result[y, index, 0] = out_real.astype(jnp.bfloat16)
        result[y, index, 1] = out_imag.astype(jnp.bfloat16)

    def write(step):
        span = pl.ds(step * 2 * SBLOCK, 2 * SBLOCK)
        return pltpu.make_async_copy(result.at[:, span], out_ref.at[:, span], sems.at[step])

    def block(step, carry):
        first = step * 2 * SBLOCK
        for current, following in ((0, 1), (1, 0)):
            for local in range(SBLOCK):
                index = first + current * SBLOCK + local
                ahead = jnp.minimum(index + SBLOCK, slices - 1)
                unpack(ahead, buffers[following], local)
                for y in range(2):
                    one(index, y, buffers[current], local)
        write(step).start()
        return carry

    steps = slices // (2 * SBLOCK)
    for local in range(SBLOCK):
        unpack(local, buffers[0], local)
    lax.fori_loop(0, steps, block, 0)
    for step in range(steps):
        write(step).wait()


def apply_rows(half, rows, maps):
    slices = rows.shape[0]
    width = maps.shape[0]
    shape = (width, slices, 2, COILS // 2, IMG)
    return pl.pallas_call(
        apply_kernel,
        in_specs=[pl.BlockSpec(memory_space=pltpu.SMEM)]
        + [pl.BlockSpec(memory_space=pltpu.VMEM)] * 3,
        out_specs=pl.BlockSpec(memory_space=pltpu.HBM),
        out_shape=jax.ShapeDtypeStruct(shape, jnp.bfloat16),
        scratch_shapes=[
            pltpu.VMEM(shape, jnp.bfloat16),
            pltpu.VMEM((SBLOCK, SPAN * COILS // 2, LANES), jnp.bfloat16),
            pltpu.VMEM((SBLOCK, SPAN * COILS // 2, LANES), jnp.bfloat16),
            pltpu.SemaphoreType.DMA((slices // (2 * SBLOCK),)),
        ],
        compiler_params=pltpu.CompilerParams(vmem_limit_bytes=16 * 2**20),
        name="apply_rows",
    )(half, rows, maps, jnp.asarray(phase_table()))


def shards(basis, picks, coil_maps):
    half = lax.axis_index("col").astype(jnp.int32).reshape(1)
    keep, send = partial_kernels(half, basis[0], picks)
    got = lax.ppermute(send, "col", [(0, 1), (1, 0)])
    rows = column_rows(half, keep, got)
    rows = lax.all_to_all(rows, "slc", split_axis=0, concat_axis=0, tiled=True)
    return apply_rows(half, rows, coil_maps)


def solution(mesh):
    placed = (P("slc", None, None, "col"), P("slc", "col"), P("slc", None, None, None, None))
    return jax.shard_map(
        shards,
        mesh=mesh,
        in_specs=placed,
        out_specs=P("slc", None, None, "col", None),
        check_vma=False,
    )
```
